64 devices in a mesh: dp: 8 (over x, y, core), tp: 8 (over z).
Axes of the slice: x: 2, y: 2, z: 8, core: 2. Of those that a mesh axis runs over, the one named last changes fastest.
The devices are a block of a 4x4x8 slice.
Arguments:
- x: bfloat16 [512, 2048], P('dp'), parts along dimension 0
- k_cache: bfloat16 [512, 1024, 32, 64], P('dp', None, 'tp'), parts along dimension 0
- v_cache: bfloat16 [512, 1024, 32, 64], P('dp', None, 'tp'), parts along dimension 0
- gain_a: bfloat16 [2048], replicated
- wq: bfloat16 [2048, 2048], P(None, 'tp')
- wo: bfloat16 [2048, 2048], P('tp')
- gain_m: bfloat16 [2048], replicated
- w_gate: bfloat16 [2048, 5120], P(None, 'tp')
- w_up: bfloat16 [2048, 5120], P(None, 'tp')
- w_down: bfloat16 [5120, 2048], P('tp')
Outputs:
- output: bfloat16 [512, 2048], P('dp'), parts along dimension 0
There are 8 independent parts. The reference program is written for one: setup_inputs(seed, part) draws one part's arguments, and reference() takes and returns one part's arrays. A program takes and returns all parts, laid end to end along the dimension named above; an argument that names none is the same for every part.
All inputs are finite; a program needn't handle non-finite values.
Results may differ from the reference program's by a relative error of at most 0.017.
Values are sent between devices in bfloat16 or wider.
A program may use at most 768 MiB of HBM per device.

```python
import jax
import jax.numpy as jnp
from jax import lax

BATCH = 64
CACHE = 1024
D = 2048
HEADS = 32
KV_HEADS = 32
HEAD = 64
FF = 5120
THETA = 10000


def setup_inputs(seed: int = 0, part: int = 0) -> dict:
    kx, kc, kw, kn, kq, ko, km, kg, ku, kd = jax.random.split(jax.random.key(seed), 10)
    kx, kc, kw = (jax.random.fold_in(k, part) for k in (kx, kc, kw))

    def weights(key, rows, columns):
        return jax.random.normal(key, (rows, columns), jnp.float32) * rows**-0.5

    drawn = {
        "x": jax.random.normal(kx, (BATCH, D), jnp.float32),
        "k_cache": 2 * jax.random.normal(kc, (BATCH, CACHE, KV_HEADS, HEAD), jnp.float32),
        "v_cache": 4 * jax.random.normal(kw, (BATCH, CACHE, KV_HEADS, HEAD), jnp.float32),
        "gain_a": 1 + 0.1 * jax.random.normal(kn, (D,), jnp.float32),
        "wq": 2 * weights(kq, D, HEADS * HEAD),
        "wo": weights(ko, HEADS * HEAD, D),
        "gain_m": 1 + 0.1 * jax.random.normal(km, (D,), jnp.float32),
        "w_gate": weights(kg, D, FF),
        "w_up": weights(ku, D, FF),
        "w_down": 2 * weights(kd, FF, D),
    }
    return {k: v.astype(jnp.bfloat16) for k, v in drawn.items()}


def normed(x, gain):
    wide = x.astype(jnp.float32)
    scale = lax.rsqrt(jnp.mean(wide * wide, -1, keepdims=True) + 1e-6)
    return (wide * scale * gain.astype(jnp.float32)).astype(jnp.bfloat16)


def turned(t, place, theta):
    half = t.shape[-1] // 2
    angle = place.astype(jnp.float32)[:, None] * theta ** (-jnp.arange(half, dtype=jnp.float32) / half)
    cos, sin = jnp.cos(angle)[:, None], jnp.sin(angle)[:, None]
    a, b = t[..., :half].astype(jnp.float32), t[..., half:].astype(jnp.float32)
    return jnp.concatenate([a * cos - b * sin, b * cos + a * sin], -1).astype(jnp.bfloat16)


def matmul(a, w):
    return jnp.dot(a, w, preferred_element_type=jnp.float32).astype(jnp.bfloat16)


def einsum(form, a, b):
    return jnp.einsum(form, a.astype(jnp.float32), b.astype(jnp.float32))


def seen_by(a, wq, k_cache, v_cache, head, theta):
    batch, cache, kv_heads = k_cache.shape[:3]
    place = jnp.full((batch,), cache - 1)
    q = turned(matmul(a, wq).reshape(batch, -1, head), place, theta).reshape(batch, kv_heads, -1, head)
    scores = einsum("bgsd,bugd->bgsu", q, k_cache) * head**-0.5
    weights = jax.nn.softmax(scores, -1).astype(jnp.bfloat16)
    return einsum("bgsu,bugd->bgsd", weights, v_cache).astype(jnp.bfloat16).reshape(batch, -1)


def hidden_of(b, w_gate, w_up):
    gate = jnp.dot(b, w_gate, preferred_element_type=jnp.float32)
    up = jnp.dot(b, w_up, preferred_element_type=jnp.float32)
    return (jax.nn.silu(gate) * up).astype(jnp.bfloat16)


def reference(x, k_cache, v_cache, gain_a, wq, wo, gain_m, w_gate, w_up, w_down):
    seen = seen_by(normed(x, gain_a), wq, k_cache, v_cache, HEAD, THETA)
    h = (x.astype(jnp.float32) + jnp.dot(seen, wo, preferred_element_type=jnp.float32)).astype(jnp.bfloat16)
    hidden = hidden_of(normed(h, gain_m), w_gate, w_up)
    return (h.astype(jnp.float32) + jnp.dot(hidden, w_down, preferred_element_type=jnp.float32)).astype(jnp.bfloat16)
```

```python
import functools

import jax
import jax.numpy as jnp
import numpy as np
from jax import lax
from jax.experimental import pallas as pl
from jax.experimental.pallas import tpu as pltpu
from jax.sharding import PartitionSpec as P

HEAD = 64
THETA = 10000
EPS = 1e-6
SEQS = 4
SLOTS = 8
MLP_AT = 11
SUM_AT = 14

F32, BF16 = jnp.float32, jnp.bfloat16
MESH = pl.DeviceIdType.MESH


def dot(a, b):
    return jnp.dot(a, b, preferred_element_type=F32)


def dot_t(a, b):
    return lax.dot_general(a, b, (((1,), (1,)), ((), ())), preferred_element_type=F32)


def normed(wide, gain):
    scale = lax.rsqrt(jnp.mean(wide * wide, -1, keepdims=True) + EPS)
    return wide * scale * gain


def kernel(
    n, heads, axis,
    x_hbm, k_hbm, v_hbm, ga_hbm, wq_hbm, wo_hbm, gm_hbm, wg_hbm, wu_hbm, wd_hbm, rope_hbm,
    y_ref,
    xs, x_own, ga, gm, rope, wq, wo, wg, wu, wd,
    kbuf, vbuf, qbd, s_ref, terms, landed, h_all, b_ref, own2, terms2, landed2, y_all,
    k_sem, v_sem, w_sem, send1, recv1, send2, recv2, send3, recv3, send4, recv4,
):
    me = lax.axis_index(axis)
    width = heads * HEAD
    rows = SEQS * heads
    batch = x_hbm.shape[0] * x_hbm.shape[1]
    steps = batch // SEQS
    parts = steps // n
    cache = k_hbm.shape[-1]

    def peer(p):
        return lax.rem(me + p, n)

    def block_of(g):
        return lax.rem(me + 1 + lax.rem(g, n), n)

    def group_of(g):
        return block_of(g) * parts + g // n

    def k_copy(g):
        return pltpu.make_async_copy(k_hbm.at[group_of(g)], kbuf.at[lax.rem(g, SLOTS)], k_sem.at[lax.rem(g, SLOTS)])

    def v_copy(g):
        return pltpu.make_async_copy(v_hbm.at[group_of(g)], vbuf.at[lax.rem(g, SLOTS)], v_sem.at[lax.rem(g, SLOTS)])

    first = [
        pltpu.make_async_copy(x_hbm, xs, w_sem.at[0]),
        pltpu.make_async_copy(ga_hbm, ga, w_sem.at[1]),
        pltpu.make_async_copy(wq_hbm, wq, w_sem.at[2]),
        pltpu.make_async_copy(rope_hbm, rope, w_sem.at[3]),
    ]
    second = [pltpu.make_async_copy(wo_hbm, wo, w_sem.at[4]), pltpu.make_async_copy(x_hbm.at[me], x_own, w_sem.at[5])]
    third = [
        pltpu.make_async_copy(wg_hbm, wg, w_sem.at[6]),
        pltpu.make_async_copy(wu_hbm, wu, w_sem.at[7]),
        pltpu.make_async_copy(wd_hbm, wd, w_sem.at[8]),
        pltpu.make_async_copy(gm_hbm, gm, w_sem.at[9]),
    ]

    for c in first:
        c.start()
    k_copy(0).start()
    v_copy(0).start()
    for c in second:
        c.start()
    for g in range(1, SLOTS):
        k_copy(g).start()
        v_copy(g).start()
    k_tail = SLOTS

    barrier = pltpu.get_barrier_semaphore()
    for p in range(1, n):
        pl.semaphore_signal(barrier, inc=1, device_id={axis: peer(p)}, device_id_type=MESH)

    for c in first:
        c.wait()
    a = normed(xs[...].reshape(batch, -1).astype(F32), ga[...].astype(F32)).astype(BF16)
    q = dot(a, wq[...]).astype(BF16).astype(F32)
    lane = lax.broadcasted_iota(jnp.int32, q.shape, 1)
    half = HEAD // 2
    low = lax.rem(lane, HEAD) < half
    other = jnp.where(low, pltpu.roll(q, width - half, 1), pltpu.roll(q, half, 1))
    q = (q * rope[0:1, :] + other * rope[1:2, :]).astype(BF16)
    r = lax.broadcasted_iota(jnp.int32, (steps * rows, batch), 0)
    t = lax.broadcasted_iota(jnp.int32, (steps * rows, batch), 1)
    pick = jnp.where(t == (r // rows) * SEQS + lax.rem(r, SEQS), 1.0, 0.0).astype(BF16)
    r = lax.broadcasted_iota(jnp.int32, (steps * rows, width), 0)
    c = lax.broadcasted_iota(jnp.int32, (steps * rows, width), 1)
    spread = jnp.where(c // HEAD == lax.rem(r // SEQS, heads), dot(pick, q), 0.0).astype(BF16)
    qbd[...] = spread.reshape(steps, rows, width)

    row = lax.broadcasted_iota(jnp.int32, (rows, cache), 0)
    vrow = lax.broadcasted_iota(jnp.int32, (width, rows), 0)
    vcol = lax.broadcasted_iota(jnp.int32, (width, rows), 1)
    fold_r = lax.broadcasted_iota(jnp.int32, (8, rows), 0)
    fold_c = lax.broadcasted_iota(jnp.int32, (8, rows), 1)
    fold = jnp.where(lax.rem(fold_c, SEQS) == fold_r, 1.0, 0.0).astype(BF16)

    def scores(g):
        slot = lax.rem(g, SLOTS)
        qs = qbd[group_of(g)]
        s = dot(qs, kbuf[slot, 0])
        for i in range(1, SEQS):
            s = jnp.where(lax.rem(row, SEQS) == i, dot(qs, kbuf[slot, i]), s)
        return s

    def weights():
        s = s_ref[...]
        e = jnp.exp((s - jnp.max(s, -1, keepdims=True)) * HEAD**-0.5)
        return (e * (1.0 / jnp.sum(e, -1, keepdims=True))).astype(BF16)

    def attended(g, w):
        slot = lax.rem(g, SLOTS)
        acc = jnp.zeros((width, rows), F32)
        for i in range(SEQS):
            acc = jnp.where(vcol == (vrow // HEAD) * SEQS + i, dot_t(vbuf[slot, i], w), acc)
        return dot_t(fold, acc.astype(BF16)).astype(BF16)

    def term1(g, to):
        return pltpu.make_async_remote_copy(
            terms.at[g], landed.at[g], send1.at[g], recv1.at[g], device_id={axis: to}, device_id_type=MESH
        )

    def gather1(b, p):
        return pltpu.make_async_remote_copy(
            h_all.at[b, me], h_all.at[b, me], send2.at[b, p], recv2.at[b, p], device_id={axis: peer(p)}, device_id_type=MESH
        )

    def term2(b, p):
        return pltpu.make_async_remote_copy(
            terms2.at[b, peer(p)], landed2.at[b, p], send3.at[b, p], recv3.at[b, p], device_id={axis: peer(p)}, device_id_type=MESH
        )

    def gather2(b, p):
        return pltpu.make_async_remote_copy(
            y_all.at[b, me], y_all.at[b, me], send4.at[b, p], recv4.at[b, p], device_id={axis: peer(p)}, device_id_type=MESH
        )

    far_first = sorted(range(1, n), key=lambda p: -min(p, n - p))

    def finish_h(b, own):
        h = x_own[...].astype(F32)[b * SEQS : (b + 1) * SEQS] + own
        for k in range(n - 1):
            term1(b * n + k, me).wait_recv()
            h = h + landed[b * n + k].astype(F32)
        h_all[b, me] = h.astype(BF16)
        for p in far_first:
            gather1(b, p).start()

    def mlp(b):
        for p in far_first:
            pltpu.make_async_remote_copy(
                h_all.at[b, peer(n - p)], h_all.at[b, peer(n - p)], send2.at[b, p], recv2.at[b, p],
                device_id={axis: peer(p)}, device_id_type=MESH,
            ).wait_recv()
        gain = gm[...].astype(F32)
        for j in range(n):
            b_ref[j * SEQS : (j + 1) * SEQS, :] = normed(h_all[b, j].astype(F32), gain)
        states = b_ref[...].astype(BF16)
        gate, up = dot(states, wg[...]), dot(states, wu[...])
        hidden = (gate * (1.0 / (1.0 + jnp.exp(-gate))) * up).astype(BF16)
        part = dot(hidden, wd[...])
        for j in range(n):
            mine = part[j * SEQS : (j + 1) * SEQS]
            own2[j] = mine
            terms2[b, j] = mine.astype(BF16)
        for p in far_first:
            term2(b, p).start()

    def finish_y(b):
        y = h_all[b, me].astype(F32) + own2[me]
        for p in far_first:
            term2(b, p).wait_recv()
            y = y + landed2[b, p].astype(F32)
        y_all[b, me] = y.astype(BF16)
        for p in far_first:
            gather2(b, p).start()

    k_copy(0).wait()
    s_ref[...] = scores(0)
    k_copy(k_tail).start()
    for c in second:
        c.wait()
    pl.semaphore_wait(barrier, n - 1)

    def body(g, carry):
        @pl.when(g == 2)
        def _():
            for c in third:
                c.start()

        if parts > 1:

            @pl.when(g == MLP_AT)
            def _():
                for c in third:
                    c.wait()
                mlp(0)

            @pl.when(g == SUM_AT)
            def _():
                finish_y(0)

        k_copy(g + 1).wait()
        v_copy(g).wait()
        w = weights()
        s = scores(g + 1)
        part = dot(attended(g, w), wo[...])[:SEQS]
        s_ref[...] = s

        @pl.when(g + 1 + SLOTS < steps)
        def _():
            k_copy(g + 1 + SLOTS).start()

        @pl.when(g + SLOTS < steps)
        def _():
            v_copy(g + SLOTS).start()

        last = lax.rem(g, n) == n - 1

        @pl.when(jnp.logical_not(last))
        def _():
            terms[g] = part.astype(BF16)
            term1(g, block_of(g)).start()

        @pl.when(last)
        def _():
            finish_h(0, part)

        return carry

    lax.fori_loop(0, steps - 1, body, 0)
    g = steps - 1
    v_copy(g).wait()
    finish_h(parts - 1, dot(attended(g, weights()), wo[...])[:SEQS])
    mlp(parts - 1)
    finish_y(parts - 1)

    for b in range(parts):
        for p in far_first:
            pltpu.make_async_remote_copy(
                y_all.at[b, peer(n - p)], y_all.at[b, peer(n - p)], send4.at[b, p], recv4.at[b, p],
                device_id={axis: peer(p)}, device_id_type=MESH,
            ).wait_recv()
    for j in range(n):
        y_ref[j] = jnp.concatenate([y_all[b, j].astype(F32) for b in range(parts)], 0).astype(BF16)

    for b in range(parts):
        for k in range(n - 1):
            term1(b * n + k, me).wait_send()
        for p in far_first:
            gather1(b, p).wait_send()
            term2(b, p).wait_send()
            gather2(b, p).wait_send()


def solution(mesh):
    n = mesh.shape["tp"]

    def step(x, k_cache, v_cache, gain_a, wq, wo, gain_m, w_gate, w_up, w_down):
        batch, d = x.shape
        cache, heads = k_cache.shape[1:3]
        width, ff = heads * HEAD, w_gate.shape[1]
        steps = batch // SEQS
        parts = steps // n

        def turned_round(c):
            return c.transpose(0, 2, 3, 1).reshape(steps, SEQS, width, cache)

        half = HEAD // 2
        angle = (cache - 1) * THETA ** (-np.arange(half, dtype=np.float64) / half)
        cos, sin = np.cos(angle), np.sin(angle)
        rope = np.stack([np.tile(np.concatenate([cos, cos]), heads), np.tile(np.concatenate([-sin, sin]), heads)])
        rope = jnp.asarray(rope.astype(np.float32))

        dma = pltpu.SemaphoreType.DMA
        out = pl.pallas_call(
            functools.partial(kernel, n, heads, "tp"),
            out_shape=jax.ShapeDtypeStruct((n, batch // n, d), BF16),
            in_specs=[pl.BlockSpec(memory_space=pl.ANY)] * 11,
            out_specs=pl.BlockSpec(memory_space=pltpu.VMEM),
            scratch_shapes=[
                pltpu.VMEM((n, batch // n, d), BF16),
                pltpu.VMEM((batch // n, d), BF16),
                pltpu.VMEM((1, d), BF16),
                pltpu.VMEM((1, d), BF16),
                pltpu.VMEM((2, width), F32),
                pltpu.VMEM(wq.shape, BF16),
                pltpu.VMEM(wo.shape, BF16),
                pltpu.VMEM(w_gate.shape, BF16),
                pltpu.VMEM(w_up.shape, BF16),
                pltpu.VMEM(w_down.shape, BF16),
                pltpu.VMEM((SLOTS, SEQS, width, cache), BF16),
                pltpu.VMEM((SLOTS, SEQS, width, cache), BF16),
                pltpu.VMEM((steps, SEQS * heads, width), BF16),
                pltpu.VMEM((SEQS * heads, cache), F32),
                pltpu.VMEM((steps, SEQS, d), BF16),
                pltpu.VMEM((steps, SEQS, d), BF16),
                pltpu.VMEM((parts, n, SEQS, d), BF16),
                pltpu.VMEM((n * SEQS, d), F32),
                pltpu.VMEM((n, SEQS, d), F32),
                pltpu.VMEM((parts, n, SEQS, d), BF16),
                pltpu.VMEM((parts, n, SEQS, d), BF16),
                pltpu.VMEM((parts, n, SEQS, d), BF16),
                dma((SLOTS,)),
                dma((SLOTS,)),
                dma((10,)),
                dma((steps,)),
                dma((steps,)),
            ]
            + [dma((parts, n))] * 6,
            compiler_params=pltpu.CompilerParams(collective_id=0, has_side_effects=True, vmem_limit_bytes=67043328),
        )(
            x.reshape(n, batch // n, d), turned_round(k_cache), turned_round(v_cache), gain_a.reshape(1, d), wq, wo,
            gain_m.reshape(1, d), w_gate, w_up, w_down, rope,
        )
        return out.reshape(batch, d)

    states, cache, columns, rows_of = P("dp", None), P("dp", None, "tp", None), P(None, "tp"), P("tp", None)
    return jax.shard_map(
        step,
        mesh=mesh,
        in_specs=(states, cache, cache, P(None), columns, rows_of, P(None), columns, columns, rows_of),
        out_specs=states,
        check_vma=False,
    )
```

```python
import functools

import jax
import jax.numpy as jnp
import numpy as np
from jax import lax
from jax.experimental import pallas as pl
from jax.experimental.pallas import tpu as pltpu
from jax.sharding import PartitionSpec as P

HEAD = 64
THETA = 10000
EPS = 1e-6
SEQS = 4
SLOTS = 4
MLP_AT = 13
TILE = 256

F32, BF16 = jnp.float32, jnp.bfloat16
MESH = pl.DeviceIdType.MESH


def dot(a, b):
    return jnp.dot(a, b, preferred_element_type=F32)


def dot_t(a, b):
    return lax.dot_general(a, b, (((1,), (1,)), ((), ())), preferred_element_type=F32)


def normed(wide, gain):
    scale = lax.rsqrt(jnp.mean(wide * wide, -1, keepdims=True) + EPS)
    return wide * scale * gain


def kernel(
    n, heads, axis,
    x_hbm, k_hbm, v_hbm, ga_hbm, wq_hbm, wo_hbm, gm_hbm, wg_hbm, wu_hbm, wd_hbm, rope_hbm,
    y_ref,
    xs, ga, gm, rope, wq, wo, wg, wu, wd,
    kbuf, vbuf, qcat, p_ref, o_ref, terms, landed, h_own, h_in, b_ref, own2, terms2, landed2, y_all,
    k_sem, v_sem, w_sem, send1, recv1, send2, recv2, send3, recv3, send4, recv4,
):
    me = lax.axis_index(axis)
    width = heads * HEAD
    rows = SEQS * heads
    batch = x_hbm.shape[0] * x_hbm.shape[1]
    steps = batch // SEQS
    parts = steps // n
    cache = k_hbm.shape[-1]
    d = x_hbm.shape[-1]

    def peer(p):
        return lax.rem(me + p, n)

    def block_of(g):
        return lax.rem(me + 1 + lax.rem(g, n), n)

    def group_of(g):
        return block_of(g) * parts + g // n

    def k_copy(g):
        return pltpu.make_async_copy(k_hbm.at[group_of(g)], kbuf.at[lax.rem(g, SLOTS)], k_sem.at[lax.rem(g, SLOTS)])

    def v_copy(g):
        return pltpu.make_async_copy(v_hbm.at[group_of(g)], vbuf.at[lax.rem(g, SLOTS)], v_sem.at[lax.rem(g, SLOTS)])

    first = [
        pltpu.make_async_copy(x_hbm, xs, w_sem.at[0]),
        pltpu.make_async_copy(ga_hbm, ga, w_sem.at[1]),
        pltpu.make_async_copy(wq_hbm, wq, w_sem.at[2]),
        pltpu.make_async_copy(rope_hbm, rope, w_sem.at[3]),
    ]
    wo_copy = pltpu.make_async_copy(wo_hbm, wo, w_sem.at[4])
    third = [
        pltpu.make_async_copy(wg_hbm, wg, w_sem.at[5]),
        pltpu.make_async_copy(wu_hbm, wu, w_sem.at[6]),
        pltpu.make_async_copy(wd_hbm, wd, w_sem.at[7]),
        pltpu.make_async_copy(gm_hbm, gm, w_sem.at[8]),
    ]

    for c in first:
        c.start()
    k_copy(0).start()
    wo_copy.start()
    v_copy(0).start()
    k_copy(1).start()

    barrier = pltpu.get_barrier_semaphore()
    for p in range(1, n):
        pl.semaphore_signal(barrier, inc=1, device_id={axis: peer(p)}, device_id_type=MESH)

    with jax.named_scope("first_wait"):
        for c in first:
            c.wait()
    v_copy(1).start()
    for g in range(2, SLOTS):
        k_copy(g).start()
        v_copy(g).start()

    a = normed(xs[...].reshape(batch, -1).astype(F32), ga[...].astype(F32)[None]).astype(BF16)
    q = dot(a, wq[...]).astype(BF16).astype(F32)
    lane = lax.broadcasted_iota(jnp.int32, q.shape, 1)
    half = HEAD // 2
    low = lax.rem(lane, HEAD) < half
    other = jnp.where(low, pltpu.roll(q, width - half, 1), pltpu.roll(q, half, 1))
    q = (q * rope[0:1, :] + other * rope[1:2, :]).astype(BF16)
    r = lax.broadcasted_iota(jnp.int32, (steps * rows, batch), 0)
    t = lax.broadcasted_iota(jnp.int32, (steps * rows, batch), 1)
    pick = jnp.where(t == (r // rows) * SEQS + lax.rem(r, SEQS), 1.0, 0.0).astype(BF16)
    r = lax.broadcasted_iota(jnp.int32, (steps * rows, width), 0)
    c = lax.broadcasted_iota(jnp.int32, (steps * rows, width), 1)
    spread = jnp.where(c // HEAD == lax.rem(r // SEQS, heads), dot(pick, q), 0.0)
    for i in range(SEQS):
        qcat[:, :, i * width : (i + 1) * width] = (
            jnp.where(lax.rem(r, SEQS) == i, spread, 0.0).astype(BF16).reshape(steps, rows, width)
        )

    row = lax.broadcasted_iota(jnp.int32, (rows, cache), 0)
    vrow = lax.broadcasted_iota(jnp.int32, (width, rows), 0)
    vcol = lax.broadcasted_iota(jnp.int32, (width, rows), 1)
    fold_r = lax.broadcasted_iota(jnp.int32, (8, rows), 0)
    fold_c = lax.broadcasted_iota(jnp.int32, (8, rows), 1)
    fold = jnp.where(lax.rem(fold_c, SEQS) == fold_r, 1.0, 0.0).astype(BF16)
    tiles = cache // TILE

    def score_pieces(g):
        slot, group = lax.rem(g, SLOTS), group_of(g)
        out = [None] * tiles

        def piece(t, i):
            x = dot(qcat[group, :, i * width : (i + 1) * width], kbuf[slot, i, :, t * TILE : (t + 1) * TILE])
            out[t] = x if out[t] is None else out[t] + x

        order = [(t, i) for u in range(0, tiles, 2) for i in range(SEQS) for t in range(u, min(u + 2, tiles))]
        return [functools.partial(piece, t, i) for t, i in order], out

    def value_pieces(g):
        slot = lax.rem(g, SLOTS)
        out = [None, None]

        def piece(c, i, t):
            x = dot_t(vbuf[slot, i, :, t * TILE : (t + 1) * TILE], p_ref[i, :, t * TILE : (t + 1) * TILE])
            out[c] = x if out[c] is None else out[c] + x

        order = [(c, c * SEQS // 2 + i, t) for i in range(SEQS // 2) for t in range(tiles) for c in range(2)]
        return [functools.partial(piece, *o) for o in order], out

    def store_weights(s):
        e = jnp.exp((s - jnp.max(s, -1, keepdims=True)) * HEAD**-0.5)
        w = e * (1.0 / jnp.sum(e, -1, keepdims=True))
        for i in range(SEQS):
            p_ref[i] = jnp.where(lax.rem(row, SEQS) == i, w, 0.0).astype(BF16)

    def folded(sums):
        acc = jnp.where(vcol // SEQS == vrow // HEAD, sums[0] + sums[1], 0.0)
        return dot_t(fold, acc.astype(BF16)).astype(BF16)

    def term1(b, k, to):
        return pltpu.make_async_remote_copy(
            terms.at[b, k], landed.at[b, k], send1.at[b], recv1.at[b], device_id={axis: to}, device_id_type=MESH
        )

    def gather1(b, p):
        return pltpu.make_async_remote_copy(
            h_own.at[b], h_in.at[b, p - 1], send2.at[b], recv2.at[b], device_id={axis: peer(p)}, device_id_type=MESH
        )

    def term2(b, p):
        return pltpu.make_async_remote_copy(
            terms2.at[b, p - 1], landed2.at[b, p - 1], send3.at[b], recv3.at[b], device_id={axis: peer(n - p)}, device_id_type=MESH
        )

    def gather2(b, p):
        return pltpu.make_async_remote_copy(
            y_all.at[b, me], y_all.at[b, me], send4.at[b], recv4.at[b], device_id={axis: peer(p)}, device_id_type=MESH
        )

    def all_of(ref, b, send, recv):
        some = ref.at[b, pl.ds(0, n - 1)]
        return pltpu.make_async_remote_copy(some, some, send.at[b], recv.at[b], device_id={axis: me}, device_id_type=MESH)

    far_first = sorted(range(1, n), key=lambda p: -min(p, n - p))

    def finish_h(b, own):
        h = xs[me].astype(F32)[b * SEQS : (b + 1) * SEQS] + own
        with jax.named_scope(f"term1_wait#b={b}"):
            all_of(landed, b, send1, recv1).wait_recv()
        for k in range(n - 1):
            h = h + landed[b, k].astype(F32)
        h_own[b] = h.astype(BF16)
        for p in far_first:
            gather1(b, p).start()

    def mlp(b):
        with jax.named_scope(f"gather1_wait#b={b}"):
            all_of(h_in, b, send2, recv2).wait_recv()
        gain = gm[...].astype(F32)[None]
        for j in range(n):
            b_ref[j * SEQS : (j + 1) * SEQS, :] = normed((h_in[b, j - 1] if j else h_own[b]).astype(F32), gain)
        states = b_ref[...].astype(BF16)
        gate, up = dot(states, wg[...]), dot(states, wu[...])
        hidden = (gate * (1.0 / (1.0 + jnp.exp(-gate))) * up).astype(BF16)
        part = dot(hidden, wd[...])
        own2[b] = part[:SEQS]
        for j in range(1, n):
            terms2[b, j - 1] = part[j * SEQS : (j + 1) * SEQS].astype(BF16)
        for p in far_first:
            term2(b, p).start()

    def finish_y(b):
        y = h_own[b].astype(F32) + own2[b]
        with jax.named_scope(f"term2_wait#b={b}"):
            all_of(landed2, b, send3, recv3).wait_recv()
        for p in range(1, n):
            y = y + landed2[b, p - 1].astype(F32)
        y_all[b, me] = y.astype(BF16)
        for p in far_first:
            gather2(b, p).start()

    with jax.named_scope("k0_wait"):
        k_copy(0).wait()
    todo, s = score_pieces(0)
    for piece in todo:
        piece()
    store_weights(jnp.concatenate(s, 1))
    o_ref[...] = jnp.zeros_like(o_ref)
    k_copy(SLOTS).start()
    with jax.named_scope("wo_wait"):
        wo_copy.wait()
    with jax.named_scope("barrier_wait"):
        pl.semaphore_wait(barrier, n - 1)

    def send_term(g, part):
        terms[g // n, lax.rem(g, n)] = part.astype(BF16)
        term1(g // n, lax.rem(g, n), block_of(g)).start()

    def body(g, carry):
        @pl.when(g == 2)
        def _():
            for c in third:
                c.start()

        if parts > 1:

            @pl.when(g == MLP_AT)
            def _():
                with jax.named_scope("third_wait"):
                    for c in third:
                        c.wait()
                mlp(0)

        with jax.named_scope("kv_wait"):
            k_copy(g + 1).wait()
            v_copy(g).wait()
        ks, s = score_pieces(g + 1)
        vs, sums = value_pieces(g)
        before = o_ref[...]
        part = []
        for j in range(len(vs)):
            for piece in ks[2 * j : 2 * j + 2]:
                piece()
            vs[j]()
            if j % 2:
                part.append(dot(before, wo[:, j // 2 * TILE : (j // 2 + 1) * TILE]))
        o_ref[...] = folded(sums)
        store_weights(jnp.concatenate(s, 1))
        part = jnp.concatenate(part, 1)[:SEQS]

        @pl.when(g + 1 + SLOTS < steps)
        def _():
            k_copy(g + 1 + SLOTS).start()

        @pl.when(g + SLOTS < steps)
        def _():
            v_copy(g + SLOTS).start()

        own_before = lax.rem(g, n) == 0

        @pl.when(jnp.logical_not(own_before))
        def _():
            send_term(g - 1, part)

        @pl.when(jnp.logical_and(own_before, g > 0))
        def _():
            finish_h(0, part)

        return carry

    lax.fori_loop(0, steps - 1, body, 0)
    g = steps - 1
    send_term(g - 1, dot(o_ref[...], wo[...])[:SEQS])
    v_copy(g).wait()
    vs, sums = value_pieces(g)
    for piece in vs:
        piece()
    finish_h(parts - 1, dot(folded(sums), wo[...])[:SEQS])
    for b in range(parts - 1):
        finish_y(b)
    mlp(parts - 1)
    finish_y(parts - 1)

    with jax.named_scope("gather2_wait"):
        for b in range(parts):
            all_of(y_all, b, send4, recv4).wait_recv()
    for j in range(n):
        y_ref[j] = jnp.concatenate([y_all[b, j].astype(F32) for b in range(parts)], 0).astype(BF16)

    with jax.named_scope("send_wait"):
        for b in range(parts):
            all_of(terms, b, send1, recv1).wait_send()
            all_of(h_in, b, send2, recv2).wait_send()
            all_of(terms2, b, send3, recv3).wait_send()
            all_of(y_all, b, send4, recv4).wait_send()


def solution(mesh):
    n = mesh.shape["tp"]

    def step(x, k_cache, v_cache, gain_a, wq, wo, gain_m, w_gate, w_up, w_down):
        batch, d = x.shape
        cache, heads = k_cache.shape[1:3]
        width, ff = heads * HEAD, w_gate.shape[1]
        steps = batch // SEQS
        parts = steps // n
        rows = SEQS * heads

        def turned_round(c):
            return c.transpose(0, 2, 3, 1).reshape(steps, SEQS, width, cache)

        half = HEAD // 2
        angle = (cache - 1) * THETA ** (-np.arange(half, dtype=np.float64) / half)
        cos, sin = np.cos(angle), np.sin(angle)
        rope = np.stack([np.tile(np.concatenate([cos, cos]), heads), np.tile(np.concatenate([-sin, sin]), heads)])
        rope = jnp.asarray(rope.astype(np.float32))

        dma = pltpu.SemaphoreType.DMA
        out = pl.pallas_call(
            functools.partial(kernel, n, heads, "tp"),
            out_shape=jax.ShapeDtypeStruct((n, batch // n, d), BF16),
            in_specs=[pl.BlockSpec(memory_space=pl.ANY)] * 11,
            out_specs=pl.BlockSpec(memory_space=pltpu.VMEM),
            scratch_shapes=[
                pltpu.VMEM((n, batch // n, d), BF16),
                pltpu.VMEM((d,), BF16),
                pltpu.VMEM((d,), BF16),
                pltpu.VMEM((2, width), F32),
                pltpu.VMEM(wq.shape, BF16),
                pltpu.VMEM(wo.shape, BF16),
                pltpu.VMEM(w_gate.shape, BF16),
                pltpu.VMEM(w_up.shape, BF16),
                pltpu.VMEM(w_down.shape, BF16),
                pltpu.VMEM((SLOTS, SEQS, width, cache), BF16),
                pltpu.VMEM((SLOTS, SEQS, width, cache), BF16),
                pltpu.VMEM((steps, rows, SEQS * width), BF16),
                pltpu.VMEM((SEQS, rows, cache), BF16),
                pltpu.VMEM((8, width), BF16),
                pltpu.VMEM((parts, n - 1, SEQS, d), BF16),
                pltpu.VMEM((parts, n - 1, SEQS, d), BF16),
                pltpu.VMEM((parts, SEQS, d), BF16),
                pltpu.VMEM((parts, n - 1, SEQS, d), BF16),
                pltpu.VMEM((n * SEQS, d), F32),
                pltpu.VMEM((parts, SEQS, d), F32),
                pltpu.VMEM((parts, n - 1, SEQS, d), BF16),
                pltpu.VMEM((parts, n - 1, SEQS, d), BF16),
                pltpu.VMEM((parts, n, SEQS, d), BF16),
                dma((SLOTS,)),
                dma((SLOTS,)),
                dma((9,)),
            ]
            + [dma((parts,))] * 8,
            compiler_params=pltpu.CompilerParams(collective_id=0, has_side_effects=True, vmem_limit_bytes=67043328),
        )(
            x.reshape(n, batch // n, d), turned_round(k_cache), turned_round(v_cache), gain_a, wq, wo,
            gain_m, w_gate, w_up, w_down, rope,
        )
        return out.reshape(batch, d)

    states, cache, columns, rows_of = P("dp", None), P("dp", None, "tp", None), P(None, "tp"), P("tp", None)
    return jax.shard_map(
        step,
        mesh=mesh,
        in_specs=(states, cache, cache, P(None), columns, rows_of, P(None), columns, columns, rows_of),
        out_specs=states,
        check_vma=False,
    )
```

```python
import functools

import jax
import jax.numpy as jnp
import numpy as np
from jax import lax
from jax.experimental import pallas as pl
from jax.experimental.pallas import tpu as pltpu
from jax.sharding import PartitionSpec as P

HEAD = 64
THETA = 10000
EPS = 1e-6
SEQS = 4
SLOTS = 4
TILE = 256
VMEM_LIMIT = 44 * 2**20

F32, BF16 = jnp.float32, jnp.bfloat16
MESH = pl.DeviceIdType.MESH


def dot(a, b):
    return jnp.dot(a, b, preferred_element_type=F32)


def dot_t(a, b):
    return lax.dot_general(a, b, (((1,), (1,)), ((), ())), preferred_element_type=F32)


def normed(wide, gain):
    scale = lax.rsqrt(jnp.mean(wide * wide, -1, keepdims=True) + EPS)
    return wide * scale * gain


def kernel(
    n, heads, axis,
    x_hbm, k_hbm, v_hbm, ga_hbm, wq_hbm, wo_hbm, gm_hbm, wg_hbm, wu_hbm, wd_hbm, rope_hbm,
    y_ref,
    xs, ga, gm, rope, wq, wo, wg, wu, wd,
    kbuf, vbuf, qcat, p_ref, o_ref, terms, landed, h_own, h_in, b_ref, own2, terms2, landed2, y_all,
    k_sem, v_sem, w_sem, send1, recv1, send2, recv2, send3, recv3, send4, recv4,
):
    me = lax.axis_index(axis)
    width = heads * HEAD
    rows = SEQS * heads
    batch = x_hbm.shape[0] * x_hbm.shape[1]
    steps = batch // SEQS
    parts = steps // n
    cache = k_hbm.shape[-1]
    d = x_hbm.shape[-1]

    def peer(p):
        return lax.rem(me + p, n)

    def block_of(g):
        return lax.rem(me + 1 + lax.rem(g, n), n)

    def group_of(g):
        return block_of(g) * parts + g // n

    def k_copy(g):
        return pltpu.make_async_copy(k_hbm.at[group_of(g)], kbuf.at[lax.rem(g, SLOTS)], k_sem.at[lax.rem(g, SLOTS)])

    def v_copy(g):
        return pltpu.make_async_copy(v_hbm.at[group_of(g)], vbuf.at[lax.rem(g, SLOTS)], v_sem.at[lax.rem(g, SLOTS)])

    first = [
        pltpu.make_async_copy(x_hbm, xs, w_sem.at[0]),
        pltpu.make_async_copy(ga_hbm, ga, w_sem.at[1]),
        pltpu.make_async_copy(wq_hbm, wq, w_sem.at[2]),
        pltpu.make_async_copy(rope_hbm, rope, w_sem.at[3]),
    ]
    wo_copy = pltpu.make_async_copy(wo_hbm, wo, w_sem.at[4])
    third = [
        pltpu.make_async_copy(wg_hbm, wg, w_sem.at[5]),
        pltpu.make_async_copy(wu_hbm, wu, w_sem.at[6]),
        pltpu.make_async_copy(wd_hbm, wd, w_sem.at[7]),
        pltpu.make_async_copy(gm_hbm, gm, w_sem.at[8]),
    ]

    for c in first:
        c.start()
    k_copy(0).start()
    wo_copy.start()
    v_copy(0).start()
    k_copy(1).start()

    barrier = pltpu.get_barrier_semaphore()
    for p in range(1, n):
        pl.semaphore_signal(barrier, inc=1, device_id={axis: peer(p)}, device_id_type=MESH)

    with jax.named_scope("first_wait"):
        for c in first:
            c.wait()
    v_copy(1).start()
    for g in range(2, SLOTS):
        k_copy(g).start()
        v_copy(g).start()

    a = normed(xs[...].reshape(batch, -1).astype(F32), ga[...].astype(F32)[None]).astype(BF16)
    q = dot(a, wq[...]).astype(BF16).astype(F32)
    lane = lax.broadcasted_iota(jnp.int32, q.shape, 1)
    half = HEAD // 2
    low = lax.rem(lane, HEAD) < half
    other = jnp.where(low, pltpu.roll(q, width - half, 1), pltpu.roll(q, half, 1))
    q = (q * rope[0:1, :] + other * rope[1:2, :]).astype(BF16)
    r = lax.broadcasted_iota(jnp.int32, (steps * rows, batch), 0)
    t = lax.broadcasted_iota(jnp.int32, (steps * rows, batch), 1)
    pick = jnp.where(t == (r // rows) * SEQS + lax.rem(r, SEQS), 1.0, 0.0).astype(BF16)
    r = lax.broadcasted_iota(jnp.int32, (steps * rows, width), 0)
    c = lax.broadcasted_iota(jnp.int32, (steps * rows, width), 1)
    spread = jnp.where(c // HEAD == lax.rem(r // SEQS, heads), dot(pick, q), 0.0)
    for i in range(SEQS):
        qcat[:, :, i * width : (i + 1) * width] = (
            jnp.where(lax.rem(r, SEQS) == i, spread, 0.0).astype(BF16).reshape(steps, rows, width)
        )

    row = lax.broadcasted_iota(jnp.int32, (rows, cache), 0)
    vrow = lax.broadcasted_iota(jnp.int32, (width, rows), 0)
    vcol = lax.broadcasted_iota(jnp.int32, (width, rows), 1)
    fold_r = lax.broadcasted_iota(jnp.int32, (8, rows), 0)
    fold_c = lax.broadcasted_iota(jnp.int32, (8, rows), 1)
    fold = jnp.where(lax.rem(fold_c, SEQS) == fold_r, 1.0, 0.0).astype(BF16)
    tiles = cache // TILE

    def score_pieces(g):
        slot, group = lax.rem(g, SLOTS), group_of(g)
        out = [None] * tiles

        def piece(t, i):
            x = dot(qcat[group, :, i * width : (i + 1) * width], kbuf[slot, i, :, t * TILE : (t + 1) * TILE])
            out[t] = x if out[t] is None else out[t] + x

        order = [(t, i) for u in range(0, tiles, 2) for i in range(SEQS) for t in range(u, min(u + 2, tiles))]
        return [functools.partial(piece, t, i) for t, i in order], out

    def value_pieces(g):
        slot = lax.rem(g, SLOTS)
        out = [None, None]

        def piece(c, i, t):
            x = dot_t(vbuf[slot, i, :, t * TILE : (t + 1) * TILE], p_ref[i, :, t * TILE : (t + 1) * TILE])
            out[c] = x if out[c] is None else out[c] + x

        order = [(c, c * SEQS // 2 + i, t) for i in range(SEQS // 2) for t in range(tiles) for c in range(2)]
        return [functools.partial(piece, *o) for o in order], out

    def store_weights(s):
        e = jnp.exp((s - jnp.max(s, -1, keepdims=True)) * HEAD**-0.5)
        w = e * (1.0 / jnp.sum(e, -1, keepdims=True))
        for i in range(SEQS):
            p_ref[i] = jnp.where(lax.rem(row, SEQS) == i, w, 0.0).astype(BF16)

    def folded(sums):
        acc = jnp.where(vcol // SEQS == vrow // HEAD, sums[0] + sums[1], 0.0)
        return dot_t(fold, acc.astype(BF16)).astype(BF16)

    def term1(b, k, to):
        return pltpu.make_async_remote_copy(
            terms.at[b, k], landed.at[b, k], send1.at[b], recv1.at[b], device_id={axis: to}, device_id_type=MESH
        )

    def gather1(b, p):
        return pltpu.make_async_remote_copy(
            h_own.at[b], h_in.at[b, p - 1], send2.at[b], recv2.at[b], device_id={axis: peer(p)}, device_id_type=MESH
        )

    def term2(b, p):
        return pltpu.make_async_remote_copy(
            terms2.at[b, p - 1], landed2.at[b, p - 1], send3.at[b], recv3.at[b], device_id={axis: peer(n - p)}, device_id_type=MESH
        )

    def gather2(b, p):
        return pltpu.make_async_remote_copy(
            y_all.at[b, me], y_all.at[b, me], send4.at[b], recv4.at[b], device_id={axis: peer(p)}, device_id_type=MESH
        )

    def all_of(ref, b, send, recv):
        some = ref.at[b, pl.ds(0, n - 1)]
        return pltpu.make_async_remote_copy(some, some, send.at[b], recv.at[b], device_id={axis: me}, device_id_type=MESH)

    far_first = sorted(range(1, n), key=lambda p: -min(p, n - p))

    def finish_h(b, own):
        h = xs[me].astype(F32)[b * SEQS : (b + 1) * SEQS] + own
        with jax.named_scope(f"term1_wait#b={b}"):
            all_of(landed, b, send1, recv1).wait_recv()
        for k in range(n - 1):
            h = h + landed[b, k].astype(F32)
        h_own[b] = h.astype(BF16)
        for p in far_first:
            gather1(b, p).start()

    def mlp(b):
        with jax.named_scope("gather1_wait"):
            all_of(h_in, b, send2, recv2).wait_recv()
        gain = gm[...].astype(F32)[None]
        for j in range(n):
            b_ref[j * SEQS : (j + 1) * SEQS, :] = normed((h_in[b, j - 1] if j else h_own[b]).astype(F32), gain)
        states = b_ref[...].astype(BF16)
        gate, up = dot(states, wg[...]), dot(states, wu[...])
        hidden = (gate * (1.0 / (1.0 + jnp.exp(-gate))) * up).astype(BF16)
        part = dot(hidden, wd[...])
        own2[b] = part[:SEQS]
        for j in range(1, n):
            terms2[b, j - 1] = part[j * SEQS : (j + 1) * SEQS].astype(BF16)
        for p in far_first:
            term2(b, p).start()

    def finish_y(b):
        y = h_own[b].astype(F32) + own2[b]
        with jax.named_scope("term2_wait"):
            all_of(landed2, b, send3, recv3).wait_recv()
        for p in range(1, n):
            y = y + landed2[b, p - 1].astype(F32)
        y_all[b, me] = y.astype(BF16)
        for p in far_first:
            gather2(b, p).start()

    with jax.named_scope("k0_wait"):
        k_copy(0).wait()
    todo, s = score_pieces(0)
    for piece in todo:
        piece()
    store_weights(jnp.concatenate(s, 1))
    o_ref[...] = jnp.zeros_like(o_ref)
    k_copy(SLOTS).start()
    with jax.named_scope("wo_wait"):
        wo_copy.wait()
    with jax.named_scope("barrier_wait"):
        pl.semaphore_wait(barrier, n - 1)

    def send_term(g, part):
        terms[g // n, lax.rem(g, n)] = part.astype(BF16)
        term1(g // n, lax.rem(g, n), block_of(g)).start()

    def body(g, carry):
        @pl.when(g == steps - SLOTS)
        def _():
            for c in third:
                c.start()

        with jax.named_scope("kv_wait"):
            k_copy(g + 1).wait()
            v_copy(g).wait()
        ks, s = score_pieces(g + 1)
        vs, sums = value_pieces(g)
        before = o_ref[...]
        part = []
        for j in range(len(vs)):
            for piece in ks[2 * j : 2 * j + 2]:
                piece()
            vs[j]()
            if j % 2:
                part.append(dot(before, wo[:, j // 2 * TILE : (j // 2 + 1) * TILE]))
        o_ref[...] = folded(sums)
        store_weights(jnp.concatenate(s, 1))
        part = jnp.concatenate(part, 1)[:SEQS]

        @pl.when(g + 1 + SLOTS < steps)
        def _():
            k_copy(g + 1 + SLOTS).start()

        @pl.when(g + SLOTS < steps)
        def _():
            v_copy(g + SLOTS).start()

        own_before = lax.rem(g, n) == 0

        @pl.when(jnp.logical_not(own_before))
        def _():
            send_term(g - 1, part)

        @pl.when(jnp.logical_and(own_before, g > 0))
        def _():
            finish_h(0, part)

        return carry

    lax.fori_loop(0, steps - 1, body, 0)
    g = steps - 1

    @pl.when(me >= 0)
    def _():
        send_term(g - 1, dot(o_ref[...], wo[...])[:SEQS])
        with jax.named_scope("last_v_wait"):
            v_copy(g).wait()

    @pl.when(me < n)
    def _():
        vs, sums = value_pieces(g)
        for piece in vs:
            piece()
        o_ref[...] = folded(sums)

    @pl.when(me > -1)
    def _():
        finish_h(parts - 1, dot(o_ref[...], wo[...])[:SEQS])

    with jax.named_scope("third_wait"):
        for c in third:
            c.wait()

    def each_mlp(b, carry):
        mlp(b)
        return carry

    def each_y(b, carry):
        finish_y(b)
        return carry

    lax.fori_loop(0, parts, each_mlp, 0)
    lax.fori_loop(0, parts, each_y, 0)

    with jax.named_scope("gather2_wait"):
        for b in range(parts):
            all_of(y_all, b, send4, recv4).wait_recv()
    for j in range(n):
        y_ref[j] = jnp.concatenate([y_all[b, j].astype(F32) for b in range(parts)], 0).astype(BF16)

    with jax.named_scope("send_wait"):
        for b in range(parts):
            all_of(terms, b, send1, recv1).wait_send()
            all_of(h_in, b, send2, recv2).wait_send()
            all_of(terms2, b, send3, recv3).wait_send()
            all_of(y_all, b, send4, recv4).wait_send()


def solution(mesh):
    n = mesh.shape["tp"]

    def step(x, k_cache, v_cache, gain_a, wq, wo, gain_m, w_gate, w_up, w_down):
        batch, d = x.shape
        cache, heads = k_cache.shape[1:3]
        width, ff = heads * HEAD, w_gate.shape[1]
        steps = batch // SEQS
        parts = steps // n
        rows = SEQS * heads

        def turned_round(c):
            return c.transpose(0, 2, 3, 1).reshape(steps, SEQS, width, cache)

        half = HEAD // 2
        angle = (cache - 1) * THETA ** (-np.arange(half, dtype=np.float64) / half)
        cos, sin = np.cos(angle), np.sin(angle)
        rope = np.stack([np.tile(np.concatenate([cos, cos]), heads), np.tile(np.concatenate([-sin, sin]), heads)])
        rope = jnp.asarray(rope.astype(np.float32))

        dma = pltpu.SemaphoreType.DMA
        out = pl.pallas_call(
            functools.partial(kernel, n, heads, "tp"),
            out_shape=jax.ShapeDtypeStruct((n, batch // n, d), BF16),
            in_specs=[pl.BlockSpec(memory_space=pl.ANY)] * 11,
            out_specs=pl.BlockSpec(memory_space=pltpu.VMEM),
            scratch_shapes=[
                pltpu.VMEM((n, batch // n, d), BF16),
                pltpu.VMEM((d,), BF16),
                pltpu.VMEM((d,), BF16),
                pltpu.VMEM((2, width), F32),
                pltpu.VMEM(wq.shape, BF16),
                pltpu.VMEM(wo.shape, BF16),
                pltpu.VMEM(w_gate.shape, BF16),
                pltpu.VMEM(w_up.shape, BF16),
                pltpu.VMEM(w_down.shape, BF16),
                pltpu.VMEM((SLOTS, SEQS, width, cache), BF16),
                pltpu.VMEM((SLOTS, SEQS, width, cache), BF16),
                pltpu.VMEM((steps, rows, SEQS * width), BF16),
                pltpu.VMEM((SEQS, rows, cache), BF16),
                pltpu.VMEM((8, width), BF16),
                pltpu.VMEM((parts, n - 1, SEQS, d), BF16),
                pltpu.VMEM((parts, n - 1, SEQS, d), BF16),
                pltpu.VMEM((parts, SEQS, d), BF16),
                pltpu.VMEM((parts, n - 1, SEQS, d), BF16),
                pltpu.VMEM((n * SEQS, d), F32),
                pltpu.VMEM((parts, SEQS, d), F32),
                pltpu.VMEM((parts, n - 1, SEQS, d), BF16),
                pltpu.VMEM((parts, n - 1, SEQS, d), BF16),
                pltpu.VMEM((parts, n, SEQS, d), BF16),
                dma((SLOTS,)),
                dma((SLOTS,)),
                dma((9,)),
            ]
            + [dma((parts,))] * 8,
            compiler_params=pltpu.CompilerParams(collective_id=0, has_side_effects=True, vmem_limit_bytes=VMEM_LIMIT),
        )(
            *(
                pltpu.with_memory_space_constraint(t, pltpu.HBM)
                for t in (
                    x.reshape(n, batch // n, d), turned_round(k_cache), turned_round(v_cache), gain_a, wq, wo, gain_m,
                    w_gate, w_up, w_down, rope,
                )
            )
        )
        return out.reshape(batch, d)

    states, cache, columns, rows_of = P("dp", None), P("dp", None, "tp", None), P(None, "tp"), P("tp", None)
    return jax.shard_map(
        step,
        mesh=mesh,
        in_specs=(states, cache, cache, P(None), columns, rows_of, P(None), columns, columns, rows_of),
        out_specs=states,
        check_vma=False,
    )
```

```python
import functools

import jax
import jax.numpy as jnp
import numpy as np
from jax import lax
from jax.experimental import pallas as pl
from jax.experimental.pallas import tpu as pltpu
from jax.sharding import PartitionSpec as P

HEAD = 64
THETA = 10000
EPS = 1e-6
SEQS = 4
SLOTS = 4
TILE = 256
MLP_AT = 13
VMEM_LIMIT = 44 * 2**20

F32, BF16 = jnp.float32, jnp.bfloat16
MESH = pl.DeviceIdType.MESH


def dot(a, b):
    return jnp.dot(a, b, preferred_element_type=F32)


def dot_t(a, b):
    return lax.dot_general(a, b, (((1,), (1,)), ((), ())), preferred_element_type=F32)


def normed(wide, gain):
    scale = lax.rsqrt(jnp.mean(wide * wide, -1, keepdims=True) + EPS)
    return wide * scale * gain


def kernel(
    n, heads, axis,
    x_hbm, k_hbm, v_hbm, ga_hbm, wq_hbm, wo_hbm, gm_hbm, wg_hbm, wu_hbm, wd_hbm, rope_hbm,
    y_ref,
    xs, ga, gm, rope, wq, wo, wg, wu, wd,
    kbuf, vbuf, qcat, p_ref, o_ref, terms, landed, h_own, b_own, b_in, b_ref, own2, terms2, landed2, y_all,
    k_sem, v_sem, w_sem, send1, recv1, send2, recv2, send3, recv3, send4, recv4,
):
    me = lax.axis_index(axis)
    width = heads * HEAD
    rows = SEQS * heads
    batch = x_hbm.shape[0] * x_hbm.shape[1]
    steps = batch // SEQS
    parts = steps // n
    cache = k_hbm.shape[-1]
    d = x_hbm.shape[-1]

    def peer(p):
        return lax.rem(me + p, n)

    def block_of(g):
        return lax.rem(me + 1 + lax.rem(g, n), n)

    def group_of(g):
        return block_of(g) * parts + g // n

    def k_copy(g):
        return pltpu.make_async_copy(k_hbm.at[group_of(g)], kbuf.at[lax.rem(g, SLOTS)], k_sem.at[lax.rem(g, SLOTS)])

    def v_copy(g):
        return pltpu.make_async_copy(v_hbm.at[group_of(g)], vbuf.at[lax.rem(g, SLOTS)], v_sem.at[lax.rem(g, SLOTS)])

    first = [
        pltpu.make_async_copy(x_hbm, xs, w_sem.at[0]),
        pltpu.make_async_copy(ga_hbm, ga, w_sem.at[1]),
        pltpu.make_async_copy(wq_hbm, wq, w_sem.at[2]),
        pltpu.make_async_copy(rope_hbm, rope, w_sem.at[3]),
        pltpu.make_async_copy(gm_hbm, gm, w_sem.at[8]),
    ]
    wo_copy = pltpu.make_async_copy(wo_hbm, wo, w_sem.at[4])
    third = [
        pltpu.make_async_copy(wg_hbm, wg, w_sem.at[5]),
        pltpu.make_async_copy(wu_hbm, wu, w_sem.at[6]),
        pltpu.make_async_copy(wd_hbm, wd, w_sem.at[7]),
    ]

    for c in first:
        c.start()
    k_copy(0).start()
    wo_copy.start()
    v_copy(0).start()
    k_copy(1).start()

    barrier = pltpu.get_barrier_semaphore()
    for p in range(1, n):
        pl.semaphore_signal(barrier, inc=1, device_id={axis: peer(p)}, device_id_type=MESH)

    with jax.named_scope("first_wait"):
        for c in first:
            c.wait()
    v_copy(1).start()
    for g in range(2, SLOTS):
        k_copy(g).start()
        v_copy(g).start()

    a = normed(xs[...].reshape(batch, -1).astype(F32), ga[...].astype(F32)[None]).astype(BF16)
    q = dot(a, wq[...]).astype(BF16).astype(F32)
    lane = lax.broadcasted_iota(jnp.int32, q.shape, 1)
    half = HEAD // 2
    low = lax.rem(lane, HEAD) < half
    other = jnp.where(low, pltpu.roll(q, width - half, 1), pltpu.roll(q, half, 1))
    q = (q * rope[0:1, :] + other * rope[1:2, :]).astype(BF16)
    r = lax.broadcasted_iota(jnp.int32, (steps * rows, batch), 0)
    t = lax.broadcasted_iota(jnp.int32, (steps * rows, batch), 1)
    pick = jnp.where(t == (r // rows) * SEQS + lax.rem(r, SEQS), 1.0, 0.0).astype(BF16)
    r = lax.broadcasted_iota(jnp.int32, (steps * rows, width), 0)
    c = lax.broadcasted_iota(jnp.int32, (steps * rows, width), 1)
    spread = jnp.where(c // HEAD == lax.rem(r // SEQS, heads), dot(pick, q), 0.0)
    for i in range(SEQS):
        qcat[:, :, i * width : (i + 1) * width] = (
            jnp.where(lax.rem(r, SEQS) == i, spread, 0.0).astype(BF16).reshape(steps, rows, width)
        )

    row = lax.broadcasted_iota(jnp.int32, (rows, cache), 0)
    vrow = lax.broadcasted_iota(jnp.int32, (width, rows), 0)
    vcol = lax.broadcasted_iota(jnp.int32, (width, rows), 1)
    fold_r = lax.broadcasted_iota(jnp.int32, (8, rows), 0)
    fold_c = lax.broadcasted_iota(jnp.int32, (8, rows), 1)
    fold = jnp.where(lax.rem(fold_c, SEQS) == fold_r, 1.0, 0.0).astype(BF16)
    tiles = cache // TILE

    def score_pieces(g):
        slot, group = lax.rem(g, SLOTS), group_of(g)
        out = [None] * tiles

        def piece(t, i):
            x = dot(qcat[group, :, i * width : (i + 1) * width], kbuf[slot, i, :, t * TILE : (t + 1) * TILE])
            out[t] = x if out[t] is None else out[t] + x

        order = [(t, i) for u in range(0, tiles, 2) for i in range(SEQS) for t in range(u, min(u + 2, tiles))]
        return [functools.partial(piece, t, i) for t, i in order], out

    def value_pieces(g):
        slot = lax.rem(g, SLOTS)
        out = [None, None]

        def piece(c, i, t):
            x = dot_t(vbuf[slot, i, :, t * TILE : (t + 1) * TILE], p_ref[i, :, t * TILE : (t + 1) * TILE])
            out[c] = x if out[c] is None else out[c] + x

        order = [(c, c * SEQS // 2 + i, t) for i in range(SEQS // 2) for t in range(tiles) for c in range(2)]
        return [functools.partial(piece, *o) for o in order], out

    def store_weights(s):
        e = jnp.exp((s - jnp.max(s, -1, keepdims=True)) * HEAD**-0.5)
        w = e * (1.0 / jnp.sum(e, -1, keepdims=True))
        for i in range(SEQS):
            p_ref[i] = jnp.where(lax.rem(row, SEQS) == i, w, 0.0).astype(BF16)

    def folded(sums):
        acc = jnp.where(vcol // SEQS == vrow // HEAD, sums[0] + sums[1], 0.0)
        return dot_t(fold, acc.astype(BF16)).astype(BF16)

    def term1(b, k, to):
        return pltpu.make_async_remote_copy(
            terms.at[b, k], landed.at[b, k], send1.at[b], recv1.at[b], device_id={axis: to}, device_id_type=MESH
        )

    def gather1(b, p):
        return pltpu.make_async_remote_copy(
            b_own.at[b], b_in.at[b, p - 1], send2.at[b], recv2.at[b], device_id={axis: peer(p)}, device_id_type=MESH
        )

    def term2(b, p):
        return pltpu.make_async_remote_copy(
            terms2.at[b, p - 1], landed2.at[b, p - 1], send3.at[b], recv3.at[b], device_id={axis: peer(n - p)}, device_id_type=MESH
        )

    def gather2(b, p):
        return pltpu.make_async_remote_copy(
            y_all.at[b, me], y_all.at[b, me], send4.at[b], recv4.at[b], device_id={axis: peer(p)}, device_id_type=MESH
        )

    def all_of(ref, b, send, recv):
        some = ref.at[b, pl.ds(0, n - 1)]
        return pltpu.make_async_remote_copy(some, some, send.at[b], recv.at[b], device_id={axis: me}, device_id_type=MESH)

    far_first = sorted(range(1, n), key=lambda p: -min(p, n - p))

    def finish_h(b, own):
        h = xs[me].astype(F32)[b * SEQS : (b + 1) * SEQS] + own
        with jax.named_scope(f"term1_wait#b={b}"):
            all_of(landed, b, send1, recv1).wait_recv()
        for k in range(n - 1):
            h = h + landed[b, k].astype(F32)
        h = h.astype(BF16)
        h_own[b] = h
        b_own[b] = normed(h.astype(F32), gm[...].astype(F32)[None]).astype(BF16)
        for p in far_first:
            gather1(b, p).start()

    def wait_states(b):
        with jax.named_scope("gather1_wait"):
            all_of(b_in, b, send2, recv2).wait_recv()

    def mlp(b):
        for j in range(n):
            b_ref[j * SEQS : (j + 1) * SEQS, :] = (b_in[b, j - 1] if j else b_own[b]).astype(F32)
        states = b_ref[...].astype(BF16)
        gate, up = dot(states, wg[...]), dot(states, wu[...])
        hidden = (gate * (1.0 / (1.0 + jnp.exp(-gate))) * up).astype(BF16)
        part = dot(hidden, wd[...])
        own2[b] = part[:SEQS]
        for j in range(1, n):
            terms2[b, j - 1] = part[j * SEQS : (j + 1) * SEQS].astype(BF16)
        for p in far_first:
            term2(b, p).start()

    def finish_y(b):
        y = h_own[b].astype(F32) + own2[b]
        with jax.named_scope("term2_wait"):
            all_of(landed2, b, send3, recv3).wait_recv()
        for p in range(1, n):
            y = y + landed2[b, p - 1].astype(F32)
        y_all[b, me] = y.astype(BF16)
        for p in far_first:
            gather2(b, p).start()

    with jax.named_scope("k0_wait"):
        k_copy(0).wait()
    todo, s = score_pieces(0)
    for piece in todo:
        piece()
    store_weights(jnp.concatenate(s, 1))
    o_ref[...] = jnp.zeros_like(o_ref)
    k_copy(SLOTS).start()
    with jax.named_scope("wo_wait"):
        wo_copy.wait()
    with jax.named_scope("barrier_wait"):
        pl.semaphore_wait(barrier, n - 1)

    def send_term(g, part):
        terms[g // n, lax.rem(g, n)] = part.astype(BF16)
        term1(g // n, lax.rem(g, n), block_of(g)).start()

    def body(g, carry):
        for at, c in zip((4, 6, 8), third):

            @pl.when(g == at)
            def _():
                c.start()

        if parts > 1:

            @pl.when(g == MLP_AT)
            def _():
                with jax.named_scope("third_wait"):
                    for c in third:
                        c.wait()
                wait_states(0)
                mlp(0)

        with jax.named_scope("kv_wait"):
            k_copy(g + 1).wait()
            v_copy(g).wait()
        ks, s = score_pieces(g + 1)
        vs, sums = value_pieces(g)
        before = o_ref[...]
        part = []
        for j in range(len(vs)):
            for piece in ks[2 * j : 2 * j + 2]:
                piece()
            vs[j]()
            if j % 2:
                part.append(dot(before, wo[:, j // 2 * TILE : (j // 2 + 1) * TILE]))
        o_ref[...] = folded(sums)
        store_weights(jnp.concatenate(s, 1))
        part = jnp.concatenate(part, 1)[:SEQS]

        @pl.when(g + 1 + SLOTS < steps)
        def _():
            k_copy(g + 1 + SLOTS).start()

        @pl.when(g + SLOTS < steps)
        def _():
            v_copy(g + SLOTS).start()

        own_before = lax.rem(g, n) == 0

        @pl.when(jnp.logical_not(own_before))
        def _():
            send_term(g - 1, part)

        @pl.when(jnp.logical_and(own_before, g > 0))
        def _():
            finish_h(0, part)

        return carry

    lax.fori_loop(0, steps - 1, body, 0)
    g = steps - 1

    @pl.when(me >= 0)
    def _():
        send_term(g - 1, dot(o_ref[...], wo[...])[:SEQS])
        with jax.named_scope("last_v_wait"):
            v_copy(g).wait()

    @pl.when(me < n)
    def _():
        vs, sums = value_pieces(g)
        for piece in vs:
            piece()
        o_ref[...] = folded(sums)

    @pl.when(me > -1)
    def _():
        finish_h(parts - 1, dot(o_ref[...], wo[...])[:SEQS])

    if parts == 1:
        for c in third:
            c.wait()
    wait_states(parts - 1)
    for b in range(parts - 1):
        finish_y(b)

    @pl.when(me + 1 > 0)
    def _():
        mlp(parts - 1)

    finish_y(parts - 1)

    with jax.named_scope("gather2_wait"):
        for b in range(parts):
            all_of(y_all, b, send4, recv4).wait_recv()
    for j in range(n):
        y_ref[j] = jnp.concatenate([y_all[b, j].astype(F32) for b in range(parts)], 0).astype(BF16)

    with jax.named_scope("send_wait"):
        for b in range(parts):
            all_of(terms, b, send1, recv1).wait_send()
            all_of(b_in, b, send2, recv2).wait_send()
            all_of(terms2, b, send3, recv3).wait_send()
            all_of(y_all, b, send4, recv4).wait_send()


def solution(mesh):
    n = mesh.shape["tp"]

    def step(x, k_cache, v_cache, gain_a, wq, wo, gain_m, w_gate, w_up, w_down):
        batch, d = x.shape
        cache, heads = k_cache.shape[1:3]
        width, ff = heads * HEAD, w_gate.shape[1]
        steps = batch // SEQS
        parts = steps // n
        rows = SEQS * heads

        def turned_round(c):
            return c.transpose(0, 2, 3, 1).reshape(steps, SEQS, width, cache)

        half = HEAD // 2
        angle = (cache - 1) * THETA ** (-np.arange(half, dtype=np.float64) / half)
        cos, sin = np.cos(angle), np.sin(angle)
        rope = np.stack([np.tile(np.concatenate([cos, cos]), heads), np.tile(np.concatenate([-sin, sin]), heads)])
        rope = jnp.asarray(rope.astype(np.float32))

        dma = pltpu.SemaphoreType.DMA
        out = pl.pallas_call(
            functools.partial(kernel, n, heads, "tp"),
            out_shape=jax.ShapeDtypeStruct((n, batch // n, d), BF16),
            in_specs=[pl.BlockSpec(memory_space=pl.ANY)] * 11,
            out_specs=pl.BlockSpec(memory_space=pltpu.VMEM),
            scratch_shapes=[
                pltpu.VMEM((n, batch // n, d), BF16),
                pltpu.VMEM((d,), BF16),
                pltpu.VMEM((d,), BF16),
                pltpu.VMEM((2, width), F32),
                pltpu.VMEM(wq.shape, BF16),
                pltpu.VMEM(wo.shape, BF16),
                pltpu.VMEM(w_gate.shape, BF16),
                pltpu.VMEM(w_up.shape, BF16),
                pltpu.VMEM(w_down.shape, BF16),
                pltpu.VMEM((SLOTS, SEQS, width, cache), BF16),
                pltpu.VMEM((SLOTS, SEQS, width, cache), BF16),
                pltpu.VMEM((steps, rows, SEQS * width), BF16),
                pltpu.VMEM((SEQS, rows, cache), BF16),
                pltpu.VMEM((8, width), BF16),
                pltpu.VMEM((parts, n - 1, SEQS, d), BF16),
                pltpu.VMEM((parts, n - 1, SEQS, d), BF16),
                pltpu.VMEM((parts, SEQS, d), BF16),
                pltpu.VMEM((parts, SEQS, d), BF16),
                pltpu.VMEM((parts, n - 1, SEQS, d), BF16),
                pltpu.VMEM((n * SEQS, d), F32),
                pltpu.VMEM((parts, SEQS, d), F32),
                pltpu.VMEM((parts, n - 1, SEQS, d), BF16),
                pltpu.VMEM((parts, n - 1, SEQS, d), BF16),
                pltpu.VMEM((parts, n, SEQS, d), BF16),
                dma((SLOTS,)),
                dma((SLOTS,)),
                dma((9,)),
            ]
            + [dma((parts,))] * 8,
            compiler_params=pltpu.CompilerParams(collective_id=0, has_side_effects=True, vmem_limit_bytes=VMEM_LIMIT),
        )(
            *(
                pltpu.with_memory_space_constraint(t, pltpu.HBM)
                for t in (
                    x.reshape(n, batch // n, d), turned_round(k_cache), turned_round(v_cache), gain_a, wq, wo, gain_m,
                    w_gate, w_up, w_down, rope,
                )
            )
        )
        return out.reshape(batch, d)

    states, cache, columns, rows_of = P("dp", None), P("dp", None, "tp", None), P(None, "tp"), P("tp", None)
    return jax.shard_map(
        step,
        mesh=mesh,
        in_specs=(states, cache, cache, P(None), columns, rows_of, P(None), columns, columns, rows_of),
        out_specs=states,
        check_vma=False,
    )
```

```python
import functools

import jax
import jax.numpy as jnp
import numpy as np
from jax import lax
from jax.experimental import pallas as pl
from jax.experimental.pallas import tpu as pltpu
from jax.sharding import PartitionSpec as P

HEAD = 64
THETA = 10000
EPS = 1e-6
SEQS = 4
SLOTS = 4
TILE = 256
VMEM_LIMIT = 44 * 2**20

F32, BF16 = jnp.float32, jnp.bfloat16
MESH = pl.DeviceIdType.MESH


def dot(a, b):
    return jnp.dot(a, b, preferred_element_type=F32)


def dot_t(a, b):
    return lax.dot_general(a, b, (((1,), (1,)), ((), ())), preferred_element_type=F32)


def normed(wide, gain):
    scale = lax.rsqrt(jnp.mean(wide * wide, -1, keepdims=True) + EPS)
    return wide * scale * gain


def kernel(
    n, heads, axis,
    x_hbm, k_hbm, v_hbm, ga_hbm, wq_hbm, wo_hbm, gm_hbm, wg_hbm, wu_hbm, wd_hbm, rope_hbm,
    y_ref,
    xs, ga, gm, rope, wq, wo, wg, wu, wd,
    kbuf, vbuf, qcat, p_ref, o_ref, terms, landed, h_own, b_own, b_in, b_ref, own2, terms2, landed2, y_all,
    k_sem, v_sem, w_sem, send1, recv1, send2, recv2, send3, recv3, send4, recv4,
):
    me = lax.axis_index(axis)
    width = heads * HEAD
    rows = SEQS * heads
    batch = x_hbm.shape[0] * x_hbm.shape[1]
    steps = batch // SEQS
    parts = steps // n
    cache = k_hbm.shape[-1]
    d = x_hbm.shape[-1]

    def peer(p):
        return lax.rem(me + p, n)

    def block_of(g):
        return lax.rem(me + 1 + lax.rem(g, n), n)

    def group_of(g):
        return block_of(g) * parts + g // n

    def k_copy(g):
        return pltpu.make_async_copy(k_hbm.at[group_of(g)], kbuf.at[lax.rem(g, SLOTS)], k_sem.at[lax.rem(g, SLOTS)])

    def v_copy(g):
        return pltpu.make_async_copy(v_hbm.at[group_of(g)], vbuf.at[lax.rem(g, SLOTS)], v_sem.at[lax.rem(g, SLOTS)])

    first = [
        pltpu.make_async_copy(x_hbm, xs, w_sem.at[0]),
        pltpu.make_async_copy(ga_hbm, ga, w_sem.at[1]),
        pltpu.make_async_copy(wq_hbm, wq, w_sem.at[2]),
        pltpu.make_async_copy(rope_hbm, rope, w_sem.at[3]),
        pltpu.make_async_copy(gm_hbm, gm, w_sem.at[8]),
    ]
    wo_copy = pltpu.make_async_copy(wo_hbm, wo, w_sem.at[4])
    third = [
        pltpu.make_async_copy(wg_hbm, wg, w_sem.at[5]),
        pltpu.make_async_copy(wu_hbm, wu, w_sem.at[6]),
        pltpu.make_async_copy(wd_hbm, wd, w_sem.at[7]),
    ]

    for c in first:
        c.start()
    k_copy(0).start()
    wo_copy.start()
    v_copy(0).start()
    k_copy(1).start()

    barrier = pltpu.get_barrier_semaphore()
    for p in range(1, n):
        pl.semaphore_signal(barrier, inc=1, device_id={axis: peer(p)}, device_id_type=MESH)

    with jax.named_scope("first_wait"):
        for c in first:
            c.wait()
    v_copy(1).start()
    for g in range(2, SLOTS):
        k_copy(g).start()
        v_copy(g).start()

    a = normed(xs[...].reshape(batch, -1).astype(F32), ga[...].astype(F32)[None]).astype(BF16)
    q = dot(a, wq[...]).astype(BF16).astype(F32)
    lane = lax.broadcasted_iota(jnp.int32, q.shape, 1)
    half = HEAD // 2
    low = lax.rem(lane, HEAD) < half
    other = jnp.where(low, pltpu.roll(q, width - half, 1), pltpu.roll(q, half, 1))
    q = (q * rope[0:1, :] + other * rope[1:2, :]).astype(BF16)
    r = lax.broadcasted_iota(jnp.int32, (steps * rows, batch), 0)
    t = lax.broadcasted_iota(jnp.int32, (steps * rows, batch), 1)
    pick = jnp.where(t == (r // rows) * SEQS + lax.rem(r, SEQS), 1.0, 0.0).astype(BF16)
    r = lax.broadcasted_iota(jnp.int32, (steps * rows, width), 0)
    c = lax.broadcasted_iota(jnp.int32, (steps * rows, width), 1)
    spread = jnp.where(c // HEAD == lax.rem(r // SEQS, heads), dot(pick, q), 0.0)
    for i in range(SEQS):
        qcat[:, :, i * width : (i + 1) * width] = (
            jnp.where(lax.rem(r, SEQS) == i, spread, 0.0).astype(BF16).reshape(steps, rows, width)
        )

    row = lax.broadcasted_iota(jnp.int32, (rows, cache), 0)
    vrow = lax.broadcasted_iota(jnp.int32, (width, rows), 0)
    vcol = lax.broadcasted_iota(jnp.int32, (width, rows), 1)
    fold_r = lax.broadcasted_iota(jnp.int32, (2 * SEQS, rows), 0)
    fold_c = lax.broadcasted_iota(jnp.int32, (2 * SEQS, rows), 1)
    res_r = lax.broadcasted_iota(jnp.int32, (2 * SEQS, width), 0)

    def scores(g):
        slot, group = lax.rem(g, SLOTS), group_of(g)
        columns = [pl.ds(t, TILE) for t in range(0, cache, TILE)]
        return jnp.concatenate([dot(qcat[group], kbuf[slot, :, :, c].reshape(SEQS * width, TILE)) for c in columns], 1)

    def values(g):
        slot, half = lax.rem(g, SLOTS), SEQS // 2
        sums = [None, None]
        for i in range(half):
            for c in range(2):
                x = dot_t(vbuf[slot, c * half + i], p_ref[c * half + i])
                sums[c] = x if i == 0 else sums[c] + x
        return sums

    def store_weights(s):
        e = jnp.exp((s - jnp.max(s, -1, keepdims=True)) * HEAD**-0.5)
        w = e * (1.0 / jnp.sum(e, -1, keepdims=True))
        for i in range(SEQS):
            p_ref[i] = jnp.where(lax.rem(row, SEQS) == i, w, 0.0).astype(BF16)

    def store_results(g, sums):
        odd = lax.rem(g, 2)
        acc = jnp.where(vcol // SEQS == vrow // HEAD, sums[0] + sums[1], 0.0)
        fold = jnp.where(lax.rem(fold_c, SEQS) + SEQS * odd == fold_r, 1.0, 0.0).astype(BF16)
        other = jnp.where(res_r // SEQS == odd, 0.0, o_ref[...].astype(F32))
        o_ref[...] = (other + dot_t(fold, acc.astype(BF16))).astype(BF16)

    def term1(b, k, to):
        return pltpu.make_async_remote_copy(
            terms.at[b, k], landed.at[b, k], send1.at[b], recv1.at[b], device_id={axis: to}, device_id_type=MESH
        )

    def gather1(b, p):
        return pltpu.make_async_remote_copy(
            b_own.at[b], b_in.at[b, p - 1], send2.at[b], recv2.at[b], device_id={axis: peer(p)}, device_id_type=MESH
        )

    def term2(b, p):
        return pltpu.make_async_remote_copy(
            terms2.at[b, p - 1], landed2.at[b, p - 1], send3.at[b], recv3.at[b], device_id={axis: peer(n - p)}, device_id_type=MESH
        )

    def gather2(b, p):
        return pltpu.make_async_remote_copy(
            y_all.at[b, me], y_all.at[b, me], send4.at[b], recv4.at[b], device_id={axis: peer(p)}, device_id_type=MESH
        )

    def all_of(ref, b, send, recv):
        some = ref.at[b, pl.ds(0, n - 1)]
        return pltpu.make_async_remote_copy(some, some, send.at[b], recv.at[b], device_id={axis: me}, device_id_type=MESH)

    far_first = sorted(range(1, n), key=lambda p: -min(p, n - p))

    def finish_h(b, own):
        h = xs[me].astype(F32)[b * SEQS : (b + 1) * SEQS] + own
        with jax.named_scope(f"term1_wait#b={b}"):
            all_of(landed, b, send1, recv1).wait_recv()
        for k in range(n - 1):
            h = h + landed[b, k].astype(F32)
        h = h.astype(BF16)
        h_own[b] = h
        b_own[b] = normed(h.astype(F32), gm[...].astype(F32)[None]).astype(BF16)
        for p in far_first:
            gather1(b, p).start()

    def mlp(b):
        with jax.named_scope("gather1_wait"):
            all_of(b_in, b, send2, recv2).wait_recv()
        for j in range(n):
            b_ref[j * SEQS : (j + 1) * SEQS, :] = (b_in[b, j - 1] if j else b_own[b]).astype(F32)
        states = b_ref[...].astype(BF16)
        gate, up = dot(states, wg[...]), dot(states, wu[...])
        hidden = (gate * (1.0 / (1.0 + jnp.exp(-gate))) * up).astype(BF16)
        part = dot(hidden, wd[...])
        own2[b] = part[:SEQS]
        for j in range(1, n):
            terms2[b, j - 1] = part[j * SEQS : (j + 1) * SEQS].astype(BF16)
        for p in far_first:
            term2(b, p).start()

    def finish_y(b):
        y = h_own[b].astype(F32) + own2[b]
        with jax.named_scope("term2_wait"):
            all_of(landed2, b, send3, recv3).wait_recv()
        for p in range(1, n):
            y = y + landed2[b, p - 1].astype(F32)
        y_all[b, me] = y.astype(BF16)
        for p in far_first:
            gather2(b, p).start()

    with jax.named_scope("k0_wait"):
        k_copy(0).wait()
    store_weights(scores(0))
    o_ref[...] = jnp.zeros_like(o_ref)
    k_copy(SLOTS).start()
    with jax.named_scope("wo_wait"):
        wo_copy.wait()
    with jax.named_scope("barrier_wait"):
        pl.semaphore_wait(barrier, n - 1)

    def send_term(g, part):
        terms[g // n, lax.rem(g, n)] = part.astype(BF16)
        term1(g // n, lax.rem(g, n), block_of(g)).start()

    def send_pair(g):
        part = dot(o_ref[...], wo[...])
        send_term(g - 2, part[:SEQS])

        @pl.when(lax.rem(g, n) == 0)
        def _():
            finish_h(0, part[SEQS:])

        @pl.when(lax.rem(g, n) > 0)
        def _():
            send_term(g - 1, part[SEQS:])

    def body(g, carry):
        @pl.when(g == steps - SLOTS)
        def _():
            for c in third:
                c.start()

        @pl.when(jnp.logical_and(lax.rem(g, 2) == 0, g > 0))
        def _():
            send_pair(g)

        with jax.named_scope("kv_wait"):
            k_copy(g + 1).wait()
            v_copy(g).wait()
        s = scores(g + 1)
        sums = values(g)
        store_results(g, sums)
        store_weights(s)

        @pl.when(g + 1 + SLOTS < steps)
        def _():
            k_copy(g + 1 + SLOTS).start()

        @pl.when(g + SLOTS < steps)
        def _():
            v_copy(g + SLOTS).start()

        return carry

    lax.fori_loop(0, steps - 2, body, 0)
    g = steps - 2

    @pl.when(me >= 0)
    def _():
        send_pair(g)
        with jax.named_scope("last_wait"):
            v_copy(g).wait()

    @pl.when(me < n)
    def _():
        store_results(g, values(g))

    @pl.when(me > -1)
    def _():
        send_term(g, dot(o_ref[...], wo[...])[:SEQS])
        with jax.named_scope("last_wait"):
            k_copy(g + 1).wait()
            v_copy(g + 1).wait()

    @pl.when(me < n + 1)
    def _():
        store_weights(scores(g + 1))

    @pl.when(me > -2)
    def _():
        store_results(g + 1, values(g + 1))

    @pl.when(me < n + 2)
    def _():
        finish_h(parts - 1, dot(o_ref[...], wo[...])[SEQS:])

    with jax.named_scope("third_wait"):
        for c in third:
            c.wait()

    def each_mlp(b, carry):
        mlp(b)
        return carry

    def each_y(b, carry):
        finish_y(b)
        return carry

    lax.fori_loop(0, parts, each_mlp, 0)
    lax.fori_loop(0, parts, each_y, 0)

    with jax.named_scope("gather2_wait"):
        for b in range(parts):
            all_of(y_all, b, send4, recv4).wait_recv()
    for j in range(n):
        y_ref[j] = jnp.concatenate([y_all[b, j].astype(F32) for b in range(parts)], 0).astype(BF16)

    with jax.named_scope("send_wait"):
        for b in range(parts):
            all_of(terms, b, send1, recv1).wait_send()
            all_of(b_in, b, send2, recv2).wait_send()
            all_of(terms2, b, send3, recv3).wait_send()
            all_of(y_all, b, send4, recv4).wait_send()


def solution(mesh):
    n = mesh.shape["tp"]

    def step(x, k_cache, v_cache, gain_a, wq, wo, gain_m, w_gate, w_up, w_down):
        batch, d = x.shape
        cache, heads = k_cache.shape[1:3]
        width, ff = heads * HEAD, w_gate.shape[1]
        steps = batch // SEQS
        parts = steps // n
        rows = SEQS * heads

        def turned_round(c):
            return c.transpose(0, 2, 3, 1).reshape(steps, SEQS, width, cache)

        half = HEAD // 2
        angle = (cache - 1) * THETA ** (-np.arange(half, dtype=np.float64) / half)
        cos, sin = np.cos(angle), np.sin(angle)
        rope = np.stack([np.tile(np.concatenate([cos, cos]), heads), np.tile(np.concatenate([-sin, sin]), heads)])
        rope = jnp.asarray(rope.astype(np.float32))

        dma = pltpu.SemaphoreType.DMA
        out = pl.pallas_call(
            functools.partial(kernel, n, heads, "tp"),
            out_shape=jax.ShapeDtypeStruct((n, batch // n, d), BF16),
            in_specs=[pl.BlockSpec(memory_space=pl.ANY)] * 11,
            out_specs=pl.BlockSpec(memory_space=pltpu.VMEM),
            scratch_shapes=[
                pltpu.VMEM((n, batch // n, d), BF16),
                pltpu.VMEM((d,), BF16),
                pltpu.VMEM((d,), BF16),
                pltpu.VMEM((2, width), F32),
                pltpu.VMEM(wq.shape, BF16),
                pltpu.VMEM(wo.shape, BF16),
                pltpu.VMEM(w_gate.shape, BF16),
                pltpu.VMEM(w_up.shape, BF16),
                pltpu.VMEM(w_down.shape, BF16),
                pltpu.VMEM((SLOTS, SEQS, width, cache), BF16),
                pltpu.VMEM((SLOTS, SEQS, width, cache), BF16),
                pltpu.VMEM((steps, rows, SEQS * width), BF16),
                pltpu.VMEM((SEQS, rows, cache), BF16),
                pltpu.VMEM((2 * SEQS, width), BF16),
                pltpu.VMEM((parts, n - 1, SEQS, d), BF16),
                pltpu.VMEM((parts, n - 1, SEQS, d), BF16),
                pltpu.VMEM((parts, SEQS, d), BF16),
                pltpu.VMEM((parts, SEQS, d), BF16),
                pltpu.VMEM((parts, n - 1, SEQS, d), BF16),
                pltpu.VMEM((n * SEQS, d), F32),
                pltpu.VMEM((parts, SEQS, d), F32),
                pltpu.VMEM((parts, n - 1, SEQS, d), BF16),
                pltpu.VMEM((parts, n - 1, SEQS, d), BF16),
                pltpu.VMEM((parts, n, SEQS, d), BF16),
                dma((SLOTS,)),
                dma((SLOTS,)),
                dma((9,)),
            ]
            + [dma((parts,))] * 8,
            compiler_params=pltpu.CompilerParams(collective_id=0, has_side_effects=True, vmem_limit_bytes=VMEM_LIMIT),
        )(
            *(
                pltpu.with_memory_space_constraint(t, pltpu.HBM)
                for t in (
                    x.reshape(n, batch // n, d), turned_round(k_cache), turned_round(v_cache), gain_a, wq, wo, gain_m,
                    w_gate, w_up, w_down, rope,
                )
            )
        )
        return out.reshape(batch, d)

    states, cache, columns, rows_of = P("dp", None), P("dp", None, "tp", None), P(None, "tp"), P("tp", None)
    return jax.shard_map(
        step,
        mesh=mesh,
        in_specs=(states, cache, cache, P(None), columns, rows_of, P(None), columns, columns, rows_of),
        out_specs=states,
        check_vma=False,
    )
```

```python
import functools

import jax
import jax.numpy as jnp
import numpy as np
from jax import lax
from jax.experimental import pallas as pl
from jax.experimental.pallas import tpu as pltpu
from jax.sharding import PartitionSpec as P

HEAD = 64
THETA = 10000
EPS = 1e-6
SEQS = 4
SLOTS = 4
TILE = 256
VMEM_LIMIT = 44 * 2**20

F32, BF16 = jnp.float32, jnp.bfloat16
MESH = pl.DeviceIdType.MESH


def dot(a, b):
    return jnp.dot(a, b, preferred_element_type=F32)


def dot_t(a, b):
    return lax.dot_general(a, b, (((1,), (1,)), ((), ())), preferred_element_type=F32)


def normed(wide, gain):
    scale = lax.rsqrt(jnp.mean(wide * wide, -1, keepdims=True) + EPS)
    return wide * scale * gain


def kernel(
    n, heads, axis,
    x_hbm, k_hbm, v_hbm, ga_hbm, wq_hbm, wo_hbm, gm_hbm, wg_hbm, wu_hbm, wd_hbm, rope_hbm,
    y_ref,
    xs, ga, gm, rope, wq, wo, wg, wu, wd,
    kbuf, vbuf, qcat, p_ref, o_ref, terms, landed, h_own, b_own, b_in, b_ref, own2, terms2, landed2, y_all,
    k_sem, v_sem, w_sem, send1, recv1, send2, recv2, send3, recv3, send4, recv4,
):
    me = lax.axis_index(axis)
    width = heads * HEAD
    rows = SEQS * heads
    batch = x_hbm.shape[0] * x_hbm.shape[1]
    steps = batch // SEQS
    parts = steps // n
    cache = k_hbm.shape[-1]
    d = x_hbm.shape[-1]

    def peer(p):
        return lax.rem(me + p, n)

    def block_of(g):
        return lax.rem(me + 1 + lax.rem(g, n), n)

    def group_of(g):
        return block_of(g) * parts + g // n

    def k_copy(g):
        return pltpu.make_async_copy(k_hbm.at[group_of(g)], kbuf.at[lax.rem(g, SLOTS)], k_sem.at[lax.rem(g, SLOTS)])

    def v_copy(g):
        return pltpu.make_async_copy(v_hbm.at[group_of(g)], vbuf.at[lax.rem(g, SLOTS)], v_sem.at[lax.rem(g, SLOTS)])

    first = [
        pltpu.make_async_copy(x_hbm, xs, w_sem.at[0]),
        pltpu.make_async_copy(ga_hbm, ga, w_sem.at[1]),
        pltpu.make_async_copy(wq_hbm, wq, w_sem.at[2]),
        pltpu.make_async_copy(rope_hbm, rope, w_sem.at[3]),
        pltpu.make_async_copy(gm_hbm, gm, w_sem.at[8]),
    ]
    wo_copy = pltpu.make_async_copy(wo_hbm, wo, w_sem.at[4])
    third = [
        pltpu.make_async_copy(wg_hbm, wg, w_sem.at[5]),
        pltpu.make_async_copy(wu_hbm, wu, w_sem.at[6]),
        pltpu.make_async_copy(wd_hbm, wd, w_sem.at[7]),
    ]

    for c in first:
        c.start()
    k_copy(0).start()
    wo_copy.start()
    v_copy(0).start()
    k_copy(1).start()

    barrier = pltpu.get_barrier_semaphore()
    for p in range(1, n):
        pl.semaphore_signal(barrier, inc=1, device_id={axis: peer(p)}, device_id_type=MESH)

    with jax.named_scope("first_wait"):
        for c in first:
            c.wait()
    v_copy(1).start()
    for g in range(2, SLOTS):
        k_copy(g).start()
        v_copy(g).start()

    a = normed(xs[...].reshape(batch, -1).astype(F32), ga[...].astype(F32)[None]).astype(BF16)
    q = dot(a, wq[...]).astype(BF16).astype(F32)
    lane = lax.broadcasted_iota(jnp.int32, q.shape, 1)
    half = HEAD // 2
    low = lax.rem(lane, HEAD) < half
    other = jnp.where(low, pltpu.roll(q, width - half, 1), pltpu.roll(q, half, 1))
    q = (q * rope[0:1, :] + other * rope[1:2, :]).astype(BF16)
    r = lax.broadcasted_iota(jnp.int32, (steps * rows, batch), 0)
    t = lax.broadcasted_iota(jnp.int32, (steps * rows, batch), 1)
    pick = jnp.where(t == (r // rows) * SEQS + lax.rem(r, SEQS), 1.0, 0.0).astype(BF16)
    r = lax.broadcasted_iota(jnp.int32, (steps * rows, width), 0)
    c = lax.broadcasted_iota(jnp.int32, (steps * rows, width), 1)
    spread = jnp.where(c // HEAD == lax.rem(r // SEQS, heads), dot(pick, q), 0.0)
    for i in range(SEQS):
        qcat[:, :, i * width : (i + 1) * width] = (
            jnp.where(lax.rem(r, SEQS) == i, spread, 0.0).astype(BF16).reshape(steps, rows, width)
        )

    row = lax.broadcasted_iota(jnp.int32, (rows, cache), 0)
    vrow = lax.broadcasted_iota(jnp.int32, (width, rows), 0)
    vcol = lax.broadcasted_iota(jnp.int32, (width, rows), 1)
    fold_r = lax.broadcasted_iota(jnp.int32, (2 * SEQS, rows), 0)
    fold_c = lax.broadcasted_iota(jnp.int32, (2 * SEQS, rows), 1)
    tiles = cache // TILE
    res_r = lax.broadcasted_iota(jnp.int32, (2 * SEQS, width), 0)

    def scores(g):
        slot, group = lax.rem(g, SLOTS), group_of(g)
        columns = [pl.ds(t, TILE) for t in range(0, cache, TILE)]
        return jnp.concatenate([dot(qcat[group], kbuf[slot, :, :, c].reshape(SEQS * width, TILE)) for c in columns], 1)

    def values(g):
        slot, half = lax.rem(g, SLOTS), SEQS // 2
        sums = [None, None]
        for i in range(half):
            for c in range(2):
                x = dot_t(vbuf[slot, c * half + i], p_ref[c * half + i])
                sums[c] = x if i == 0 else sums[c] + x
        return sums

    def score_pieces(g):
        slot, group = lax.rem(g, SLOTS), group_of(g)
        out = [None] * tiles

        def piece(t, i):
            x = dot(qcat[group, :, i * width : (i + 1) * width], kbuf[slot, i, :, t * TILE : (t + 1) * TILE])
            out[t] = x if out[t] is None else out[t] + x

        order = [(t, i) for u in range(0, tiles, 2) for i in range(SEQS) for t in range(u, min(u + 2, tiles))]
        return [functools.partial(piece, t, i) for t, i in order], out

    def value_pieces(g):
        slot = lax.rem(g, SLOTS)
        out = [None, None]

        def piece(c, i, t):
            x = dot_t(vbuf[slot, i, :, t * TILE : (t + 1) * TILE], p_ref[i, :, t * TILE : (t + 1) * TILE])
            out[c] = x if out[c] is None else out[c] + x

        order = [(c, c * SEQS // 2 + i, t) for i in range(SEQS // 2) for t in range(tiles) for c in range(2)]
        return [functools.partial(piece, *o) for o in order], out

    def store_weights(s):
        e = jnp.exp((s - jnp.max(s, -1, keepdims=True)) * HEAD**-0.5)
        w = e * (1.0 / jnp.sum(e, -1, keepdims=True))
        for i in range(SEQS):
            p_ref[i] = jnp.where(lax.rem(row, SEQS) == i, w, 0.0).astype(BF16)

    def store_results(g, sums):
        odd = lax.rem(g, 2)
        acc = jnp.where(vcol // SEQS == vrow // HEAD, sums[0] + sums[1], 0.0)
        fold = jnp.where(lax.rem(fold_c, SEQS) + SEQS * odd == fold_r, 1.0, 0.0).astype(BF16)
        other = jnp.where(res_r // SEQS == odd, 0.0, o_ref[...].astype(F32))
        o_ref[...] = (other + dot_t(fold, acc.astype(BF16))).astype(BF16)

    def term1(b, k, to):
        return pltpu.make_async_remote_copy(
            terms.at[b, k], landed.at[b, k], send1.at[b], recv1.at[b], device_id={axis: to}, device_id_type=MESH
        )

    def gather1(b, p):
        return pltpu.make_async_remote_copy(
            b_own.at[b], b_in.at[b, p - 1], send2.at[b], recv2.at[b], device_id={axis: peer(p)}, device_id_type=MESH
        )

    def term2(b, p):
        return pltpu.make_async_remote_copy(
            terms2.at[b, p - 1], landed2.at[b, p - 1], send3.at[b], recv3.at[b], device_id={axis: peer(n - p)}, device_id_type=MESH
        )

    def gather2(b, p):
        return pltpu.make_async_remote_copy(
            y_all.at[b, me], y_all.at[b, me], send4.at[b], recv4.at[b], device_id={axis: peer(p)}, device_id_type=MESH
        )

    def all_of(ref, b, send, recv):
        some = ref.at[b, pl.ds(0, n - 1)]
        return pltpu.make_async_remote_copy(some, some, send.at[b], recv.at[b], device_id={axis: me}, device_id_type=MESH)

    far_first = sorted(range(1, n), key=lambda p: -min(p, n - p))

    def finish_h(b, own):
        h = xs[me].astype(F32)[b * SEQS : (b + 1) * SEQS] + own
        with jax.named_scope(f"term1_wait#b={b}"):
            all_of(landed, b, send1, recv1).wait_recv()
        for k in range(n - 1):
            h = h + landed[b, k].astype(F32)
        h = h.astype(BF16)
        h_own[b] = h
        b_own[b] = normed(h.astype(F32), gm[...].astype(F32)[None]).astype(BF16)
        for p in far_first:
            gather1(b, p).start()

    def mlp(b):
        with jax.named_scope("gather1_wait"):
            all_of(b_in, b, send2, recv2).wait_recv()
        for j in range(n):
            b_ref[j * SEQS : (j + 1) * SEQS, :] = (b_in[b, j - 1] if j else b_own[b]).astype(F32)
        states = b_ref[...].astype(BF16)
        gate, up = dot(states, wg[...]), dot(states, wu[...])
        hidden = (gate * (1.0 / (1.0 + jnp.exp(-gate))) * up).astype(BF16)
        part = dot(hidden, wd[...])
        own2[b] = part[:SEQS]
        for j in range(1, n):
            terms2[b, j - 1] = part[j * SEQS : (j + 1) * SEQS].astype(BF16)
        for p in far_first:
            term2(b, p).start()

    def finish_y(b):
        y = h_own[b].astype(F32) + own2[b]
        with jax.named_scope("term2_wait"):
            all_of(landed2, b, send3, recv3).wait_recv()
        for p in range(1, n):
            y = y + landed2[b, p - 1].astype(F32)
        y_all[b, me] = y.astype(BF16)
        for p in far_first:
            gather2(b, p).start()

    with jax.named_scope("k0_wait"):
        k_copy(0).wait()
    store_weights(scores(0))
    o_ref[...] = jnp.zeros_like(o_ref)
    k_copy(SLOTS).start()
    with jax.named_scope("wo_wait"):
        wo_copy.wait()
    with jax.named_scope("barrier_wait"):
        pl.semaphore_wait(barrier, n - 1)

    def send_term(g, part):
        terms[g // n, lax.rem(g, n)] = part.astype(BF16)
        term1(g // n, lax.rem(g, n), block_of(g)).start()

    def send_pair(g):
        part = dot(o_ref[...], wo[...])
        send_term(g - 2, part[:SEQS])

        @pl.when(lax.rem(g, n) == 0)
        def _():
            finish_h(0, part[SEQS:])

        @pl.when(lax.rem(g, n) > 0)
        def _():
            send_term(g - 1, part[SEQS:])

    def body(g, carry):
        @pl.when(g == steps - SLOTS)
        def _():
            for c in third:
                c.start()

        @pl.when(jnp.logical_and(lax.rem(g, 2) == 0, g > 0))
        def _():
            send_pair(g)

        with jax.named_scope("kv_wait"):
            k_copy(g + 1).wait()
            v_copy(g).wait()
        ks, s = score_pieces(g + 1)
        vs, sums = value_pieces(g)
        for j in range(len(vs)):
            ks[j]()
            vs[j]()
        store_results(g, sums)
        store_weights(jnp.concatenate(s, 1))

        @pl.when(g + 1 + SLOTS < steps)
        def _():
            k_copy(g + 1 + SLOTS).start()

        @pl.when(g + SLOTS < steps)
        def _():
            v_copy(g + SLOTS).start()

        return carry

    lax.fori_loop(0, steps - 1, body, 0)
    g = steps - 1

    @pl.when(me >= 0)
    def _():
        send_term(g - 1, dot(o_ref[...], wo[...])[:SEQS])
        with jax.named_scope("last_v_wait"):
            v_copy(g).wait()

    @pl.when(me < n)
    def _():
        store_results(g, values(g))

    @pl.when(me > -1)
    def _():
        finish_h(parts - 1, dot(o_ref[...], wo[...])[SEQS:])

    with jax.named_scope("third_wait"):
        for c in third:
            c.wait()

    def each_mlp(b, carry):
        mlp(b)
        return carry

    def each_y(b, carry):
        finish_y(b)
        return carry

    lax.fori_loop(0, parts, each_mlp, 0)
    lax.fori_loop(0, parts, each_y, 0)

    with jax.named_scope("gather2_wait"):
        for b in range(parts):
            all_of(y_all, b, send4, recv4).wait_recv()
    for j in range(n):
        y_ref[j] = jnp.concatenate([y_all[b, j].astype(F32) for b in range(parts)], 0).astype(BF16)

    with jax.named_scope("send_wait"):
        for b in range(parts):
            all_of(terms, b, send1, recv1).wait_send()
            all_of(b_in, b, send2, recv2).wait_send()
            all_of(terms2, b, send3, recv3).wait_send()
            all_of(y_all, b, send4, recv4).wait_send()


def solution(mesh):
    n = mesh.shape["tp"]

    def step(x, k_cache, v_cache, gain_a, wq, wo, gain_m, w_gate, w_up, w_down):
        batch, d = x.shape
        cache, heads = k_cache.shape[1:3]
        width, ff = heads * HEAD, w_gate.shape[1]
        steps = batch // SEQS
        parts = steps // n
        rows = SEQS * heads

        def turned_round(c):
            return c.transpose(0, 2, 3, 1).reshape(steps, SEQS, width, cache)

        half = HEAD // 2
        angle = (cache - 1) * THETA ** (-np.arange(half, dtype=np.float64) / half)
        cos, sin = np.cos(angle), np.sin(angle)
        rope = np.stack([np.tile(np.concatenate([cos, cos]), heads), np.tile(np.concatenate([-sin, sin]), heads)])
        rope = jnp.asarray(rope.astype(np.float32))

        dma = pltpu.SemaphoreType.DMA
        out = pl.pallas_call(
            functools.partial(kernel, n, heads, "tp"),
            out_shape=jax.ShapeDtypeStruct((n, batch // n, d), BF16),
            in_specs=[pl.BlockSpec(memory_space=pl.ANY)] * 11,
            out_specs=pl.BlockSpec(memory_space=pltpu.VMEM),
            scratch_shapes=[
                pltpu.VMEM((n, batch // n, d), BF16),
                pltpu.VMEM((d,), BF16),
                pltpu.VMEM((d,), BF16),
                pltpu.VMEM((2, width), F32),
                pltpu.VMEM(wq.shape, BF16),
                pltpu.VMEM(wo.shape, BF16),
                pltpu.VMEM(w_gate.shape, BF16),
                pltpu.VMEM(w_up.shape, BF16),
                pltpu.VMEM(w_down.shape, BF16),
                pltpu.VMEM((SLOTS, SEQS, width, cache), BF16),
                pltpu.VMEM((SLOTS, SEQS, width, cache), BF16),
                pltpu.VMEM((steps, rows, SEQS * width), BF16),
                pltpu.VMEM((SEQS, rows, cache), BF16),
                pltpu.VMEM((2 * SEQS, width), BF16),
                pltpu.VMEM((parts, n - 1, SEQS, d), BF16),
                pltpu.VMEM((parts, n - 1, SEQS, d), BF16),
                pltpu.VMEM((parts, SEQS, d), BF16),
                pltpu.VMEM((parts, SEQS, d), BF16),
                pltpu.VMEM((parts, n - 1, SEQS, d), BF16),
                pltpu.VMEM((n * SEQS, d), F32),
                pltpu.VMEM((parts, SEQS, d), F32),
                pltpu.VMEM((parts, n - 1, SEQS, d), BF16),
                pltpu.VMEM((parts, n - 1, SEQS, d), BF16),
                pltpu.VMEM((parts, n, SEQS, d), BF16),
                dma((SLOTS,)),
                dma((SLOTS,)),
                dma((9,)),
            ]
            + [dma((parts,))] * 8,
            compiler_params=pltpu.CompilerParams(collective_id=0, has_side_effects=True, vmem_limit_bytes=VMEM_LIMIT),
        )(
            *(
                pltpu.with_memory_space_constraint(t, pltpu.HBM)
                for t in (
                    x.reshape(n, batch // n, d), turned_round(k_cache), turned_round(v_cache), gain_a, wq, wo, gain_m,
                    w_gate, w_up, w_down, rope,
                )
            )
        )
        return out.reshape(batch, d)

    states, cache, columns, rows_of = P("dp", None), P("dp", None, "tp", None), P(None, "tp"), P("tp", None)
    return jax.shard_map(
        step,
        mesh=mesh,
        in_specs=(states, cache, cache, P(None), columns, rows_of, P(None), columns, columns, rows_of),
        out_specs=states,
        check_vma=False,
    )
```

```python
import functools

import jax
import jax.numpy as jnp
import numpy as np
from jax import lax
from jax.experimental import pallas as pl
from jax.experimental.pallas import tpu as pltpu
from jax.sharding import PartitionSpec as P

HEAD = 64
THETA = 10000
EPS = 1e-6
SEQS = 4
SLOTS = 4
TILE = 256
VMEM_LIMIT = 44 * 2**20

F32, BF16 = jnp.float32, jnp.bfloat16
MESH = pl.DeviceIdType.MESH


def dot(a, b):
    return jnp.dot(a, b, preferred_element_type=F32)


def dot_t(a, b):
    return lax.dot_general(a, b, (((1,), (1,)), ((), ())), preferred_element_type=F32)


def normed(wide, gain):
    scale = lax.rsqrt(jnp.mean(wide * wide, -1, keepdims=True) + EPS)
    return wide * scale * gain


def kernel(
    n, heads, axis,
    x_hbm, k_hbm, v_hbm, ga_hbm, wq_hbm, wo_hbm, gm_hbm, wg_hbm, wu_hbm, wd_hbm, rope_hbm,
    y_ref,
    xs, ga, gm, rope, wq, wo, wg, wu, wd,
    kbuf, vbuf, qcat, p_ref, o_ref, terms, landed, h_own, b_own, b_in, b_ref, own2, terms2, landed2, y_all,
    k_sem, v_sem, w_sem, send1, recv1, send2, recv2, send3, recv3, send4, recv4,
):
    me = lax.axis_index(axis)
    width = heads * HEAD
    rows = SEQS * heads
    batch = x_hbm.shape[0] * x_hbm.shape[1]
    steps = batch // SEQS
    parts = steps // n
    cache = k_hbm.shape[-1]
    d = x_hbm.shape[-1]

    def peer(p):
        return lax.rem(me + p, n)

    def block_of(g):
        return lax.rem(me + 1 + lax.rem(g, n), n)

    def group_of(g):
        return block_of(g) * parts + g // n

    def k_copy(g):
        return pltpu.make_async_copy(k_hbm.at[group_of(g)], kbuf.at[lax.rem(g, SLOTS)], k_sem.at[lax.rem(g, SLOTS)])

    def v_copy(g):
        return pltpu.make_async_copy(v_hbm.at[group_of(g)], vbuf.at[lax.rem(g, SLOTS)], v_sem.at[lax.rem(g, SLOTS)])

    first = [
        pltpu.make_async_copy(x_hbm, xs, w_sem.at[0]),
        pltpu.make_async_copy(ga_hbm, ga, w_sem.at[1]),
        pltpu.make_async_copy(wq_hbm, wq, w_sem.at[2]),
        pltpu.make_async_copy(rope_hbm, rope, w_sem.at[3]),
        pltpu.make_async_copy(gm_hbm, gm, w_sem.at[8]),
    ]
    wo_copy = pltpu.make_async_copy(wo_hbm, wo, w_sem.at[4])
    third = [
        pltpu.make_async_copy(wg_hbm, wg, w_sem.at[5]),
        pltpu.make_async_copy(wu_hbm, wu, w_sem.at[6]),
        pltpu.make_async_copy(wd_hbm, wd, w_sem.at[7]),
    ]

    for c in first:
        c.start()
    k_copy(0).start()
    wo_copy.start()
    v_copy(0).start()
    k_copy(1).start()

    barrier = pltpu.get_barrier_semaphore()
    for p in range(1, n):
        pl.semaphore_signal(barrier, inc=1, device_id={axis: peer(p)}, device_id_type=MESH)

    with jax.named_scope("first_wait"):
        for c in first:
            c.wait()
    v_copy(1).start()
    for g in range(2, SLOTS):
        k_copy(g).start()
        v_copy(g).start()

    a = normed(xs[...].reshape(batch, -1).astype(F32), ga[...].astype(F32)[None]).astype(BF16)
    q = dot(a, wq[...]).astype(BF16).astype(F32)
    lane = lax.broadcasted_iota(jnp.int32, q.shape, 1)
    half = HEAD // 2
    low = lax.rem(lane, HEAD) < half
    other = jnp.where(low, pltpu.roll(q, width - half, 1), pltpu.roll(q, half, 1))
    q = (q * rope[0:1, :] + other * rope[1:2, :]).astype(BF16)
    r = lax.broadcasted_iota(jnp.int32, (steps * rows, batch), 0)
    t = lax.broadcasted_iota(jnp.int32, (steps * rows, batch), 1)
    pick = jnp.where(t == (r // rows) * SEQS + lax.rem(r, SEQS), 1.0, 0.0).astype(BF16)
    r = lax.broadcasted_iota(jnp.int32, (steps * rows, width), 0)
    c = lax.broadcasted_iota(jnp.int32, (steps * rows, width), 1)
    spread = jnp.where(c // HEAD == lax.rem(r // SEQS, heads), dot(pick, q), 0.0)
    for i in range(SEQS):
        qcat[:, :, i * width : (i + 1) * width] = (
            jnp.where(lax.rem(r, SEQS) == i, spread, 0.0).astype(BF16).reshape(steps, rows, width)
        )

    row = lax.broadcasted_iota(jnp.int32, (rows, cache), 0)
    vrow = lax.broadcasted_iota(jnp.int32, (width, rows), 0)
    vcol = lax.broadcasted_iota(jnp.int32, (width, rows), 1)
    fold_r = lax.broadcasted_iota(jnp.int32, (8, rows), 0)
    fold_c = lax.broadcasted_iota(jnp.int32, (8, rows), 1)
    fold = jnp.where(lax.rem(fold_c, SEQS) == fold_r, 1.0, 0.0).astype(BF16)
    tiles = cache // TILE

    def score_pieces(g):
        slot, group = lax.rem(g, SLOTS), group_of(g)
        out = [None] * tiles

        def piece(t, i):
            x = dot(qcat[group, :, i * width : (i + 1) * width], kbuf[slot, i, :, t * TILE : (t + 1) * TILE])
            out[t] = x if out[t] is None else out[t] + x

        order = [(t, i) for u in range(0, tiles, 2) for i in range(SEQS) for t in range(u, min(u + 2, tiles))]
        return [functools.partial(piece, t, i) for t, i in order], out

    def value_pieces(g):
        slot = lax.rem(g, SLOTS)
        out = [None, None]

        def piece(c, i, t):
            x = dot_t(vbuf[slot, i, :, t * TILE : (t + 1) * TILE], p_ref[i, :, t * TILE : (t + 1) * TILE])
            out[c] = x if out[c] is None else out[c] + x

        order = [(c, c * SEQS // 2 + i, t) for i in range(SEQS // 2) for t in range(tiles) for c in range(2)]
        return [functools.partial(piece, *o) for o in order], out

    def store_weights(s):
        e = jnp.exp((s - jnp.max(s, -1, keepdims=True)) * HEAD**-0.5)
        w = e * (1.0 / jnp.sum(e, -1, keepdims=True))
        for i in range(SEQS):
            p_ref[i] = jnp.where(lax.rem(row, SEQS) == i, w, 0.0).astype(BF16)

    def folded(sums):
        acc = jnp.where(vcol // SEQS == vrow // HEAD, sums[0] + sums[1], 0.0)
        return dot_t(fold, acc.astype(BF16)).astype(BF16)

    def term1(b, k, to):
        return pltpu.make_async_remote_copy(
            terms.at[b, k], landed.at[b, k], send1.at[b], recv1.at[b], device_id={axis: to}, device_id_type=MESH
        )

    def gather1(b, p):
        return pltpu.make_async_remote_copy(
            b_own.at[b], b_in.at[b, p - 1], send2.at[b], recv2.at[b], device_id={axis: peer(p)}, device_id_type=MESH
        )

    def term2(b, p):
        return pltpu.make_async_remote_copy(
            terms2.at[b, p - 1], landed2.at[b, p - 1], send3.at[b], recv3.at[b], device_id={axis: peer(n - p)}, device_id_type=MESH
        )

    def gather2(b, p):
        return pltpu.make_async_remote_copy(
            y_all.at[b, me], y_all.at[b, me], send4.at[b], recv4.at[b], device_id={axis: peer(p)}, device_id_type=MESH
        )

    def all_of(ref, b, send, recv):
        some = ref.at[b, pl.ds(0, n - 1)]
        return pltpu.make_async_remote_copy(some, some, send.at[b], recv.at[b], device_id={axis: me}, device_id_type=MESH)

    far_first = sorted(range(1, n), key=lambda p: -min(p, n - p))

    def finish_h(b, own):
        h = xs[me].astype(F32)[b * SEQS : (b + 1) * SEQS] + own
        with jax.named_scope(f"term1_wait#b={b}"):
            all_of(landed, b, send1, recv1).wait_recv()
        for k in range(n - 1):
            h = h + landed[b, k].astype(F32)
        h = h.astype(BF16)
        h_own[b] = h
        b_own[b] = normed(h.astype(F32), gm[...].astype(F32)[None]).astype(BF16)
        for p in far_first:
            gather1(b, p).start()

    def mlp(b):
        with jax.named_scope("gather1_wait"):
            all_of(b_in, b, send2, recv2).wait_recv()
        for j in range(n):
            b_ref[j * SEQS : (j + 1) * SEQS, :] = (b_in[b, j - 1] if j else b_own[b]).astype(F32)
        states = b_ref[...].astype(BF16)
        gate, up = dot(states, wg[...]), dot(states, wu[...])
        hidden = (gate * (1.0 / (1.0 + jnp.exp(-gate))) * up).astype(BF16)
        part = dot(hidden, wd[...])
        own2[b] = part[:SEQS]
        for j in range(1, n):
            terms2[b, j - 1] = part[j * SEQS : (j + 1) * SEQS].astype(BF16)
        for p in far_first:
            term2(b, p).start()

    def finish_y(b):
        y = h_own[b].astype(F32) + own2[b]
        with jax.named_scope("term2_wait"):
            all_of(landed2, b, send3, recv3).wait_recv()
        for p in range(1, n):
            y = y + landed2[b, p - 1].astype(F32)
        y_all[b, me] = y.astype(BF16)
        for p in far_first:
            gather2(b, p).start()

    with jax.named_scope("k0_wait"):
        k_copy(0).wait()
    todo, s = score_pieces(0)
    for piece in todo:
        piece()
    store_weights(jnp.concatenate(s, 1))
    o_ref[...] = jnp.zeros_like(o_ref)
    k_copy(SLOTS).start()
    with jax.named_scope("wo_wait"):
        wo_copy.wait()
    with jax.named_scope("barrier_wait"):
        pl.semaphore_wait(barrier, n - 1)

    def send_term(g, part):
        terms[g // n, lax.rem(g, n)] = part.astype(BF16)
        term1(g // n, lax.rem(g, n), block_of(g)).start()

    def body(g, carry):
        @pl.when(g == steps - SLOTS)
        def _():
            for c in third:
                c.start()

        with jax.named_scope("kv_wait"):
            k_copy(g + 1).wait()
            v_copy(g).wait()
        ks, s = score_pieces(g + 1)
        vs, sums = value_pieces(g)
        before = o_ref[...]
        part = []
        for j in range(len(vs)):
            for piece in ks[2 * j : 2 * j + 2]:
                piece()
            vs[j]()
            if j % 2:
                part.append(dot(before, wo[:, j // 2 * TILE : (j // 2 + 1) * TILE]))
        o_ref[...] = folded(sums)
        store_weights(jnp.concatenate(s, 1))
        part = jnp.concatenate(part, 1)[:SEQS]

        @pl.when(g + 1 + SLOTS < steps)
        def _():
            k_copy(g + 1 + SLOTS).start()

        @pl.when(g + SLOTS < steps)
        def _():
            v_copy(g + SLOTS).start()

        own_before = lax.rem(g, n) == 0

        @pl.when(jnp.logical_not(own_before))
        def _():
            send_term(g - 1, part)

        @pl.when(jnp.logical_and(own_before, g > 0))
        def _():
            finish_h(0, part)

        return carry

    lax.fori_loop(0, steps - 2, body, 0)
    g = steps - 1

    @pl.when(me >= 0)
    def _():
        with jax.named_scope("last_wait"):
            v_copy(g - 1).wait()
        vs, sums = value_pieces(g - 1)
        part = dot(o_ref[...], wo[...])[:SEQS]
        for piece in vs:
            piece()
        o_ref[...] = folded(sums)
        send_term(g - 2, part)

    @pl.when(me < n)
    def _():
        send_term(g - 1, dot(o_ref[...], wo[...])[:SEQS])
        with jax.named_scope("last_wait"):
            k_copy(g).wait()

    @pl.when(me < n + 1)
    def _():
        ks, s = score_pieces(g)
        for piece in ks:
            piece()
        store_weights(jnp.concatenate(s, 1))
        with jax.named_scope("last_v_wait"):
            v_copy(g).wait()

    @pl.when(me > -2)
    def _():
        vs, sums = value_pieces(g)
        for piece in vs:
            piece()
        o_ref[...] = folded(sums)

    @pl.when(me > -1)
    def _():
        finish_h(parts - 1, dot(o_ref[...], wo[...])[:SEQS])

    with jax.named_scope("third_wait"):
        for c in third:
            c.wait()

    def each_mlp(b, carry):
        mlp(b)
        return carry

    def each_y(b, carry):
        finish_y(b)
        return carry

    lax.fori_loop(0, parts, each_mlp, 0)
    lax.fori_loop(0, parts, each_y, 0)

    with jax.named_scope("gather2_wait"):
        for b in range(parts):
            all_of(y_all, b, send4, recv4).wait_recv()
    for j in range(n):
        y_ref[j] = jnp.concatenate([y_all[b, j].astype(F32) for b in range(parts)], 0).astype(BF16)

    with jax.named_scope("send_wait"):
        for b in range(parts):
            all_of(terms, b, send1, recv1).wait_send()
            all_of(b_in, b, send2, recv2).wait_send()
            all_of(terms2, b, send3, recv3).wait_send()
            all_of(y_all, b, send4, recv4).wait_send()


def solution(mesh):
    n = mesh.shape["tp"]

    def step(x, k_cache, v_cache, gain_a, wq, wo, gain_m, w_gate, w_up, w_down):
        batch, d = x.shape
        cache, heads = k_cache.shape[1:3]
        width, ff = heads * HEAD, w_gate.shape[1]
        steps = batch // SEQS
        parts = steps // n
        rows = SEQS * heads

        def turned_round(c):
            return c.transpose(0, 2, 3, 1).reshape(steps, SEQS, width, cache)

        half = HEAD // 2
        angle = (cache - 1) * THETA ** (-np.arange(half, dtype=np.float64) / half)
        cos, sin = np.cos(angle), np.sin(angle)
        rope = np.stack([np.tile(np.concatenate([cos, cos]), heads), np.tile(np.concatenate([-sin, sin]), heads)])
        rope = jnp.asarray(rope.astype(np.float32))

        dma = pltpu.SemaphoreType.DMA
        out = pl.pallas_call(
            functools.partial(kernel, n, heads, "tp"),
            out_shape=jax.ShapeDtypeStruct((n, batch // n, d), BF16),
            in_specs=[pl.BlockSpec(memory_space=pl.ANY)] * 11,
            out_specs=pl.BlockSpec(memory_space=pltpu.VMEM),
            scratch_shapes=[
                pltpu.VMEM((n, batch // n, d), BF16),
                pltpu.VMEM((d,), BF16),
                pltpu.VMEM((d,), BF16),
                pltpu.VMEM((2, width), F32),
                pltpu.VMEM(wq.shape, BF16),
                pltpu.VMEM(wo.shape, BF16),
                pltpu.VMEM(w_gate.shape, BF16),
                pltpu.VMEM(w_up.shape, BF16),
                pltpu.VMEM(w_down.shape, BF16),
                pltpu.VMEM((SLOTS, SEQS, width, cache), BF16),
                pltpu.VMEM((SLOTS, SEQS, width, cache), BF16),
                pltpu.VMEM((steps, rows, SEQS * width), BF16),
                pltpu.VMEM((SEQS, rows, cache), BF16),
                pltpu.VMEM((8, width), BF16),
                pltpu.VMEM((parts, n - 1, SEQS, d), BF16),
                pltpu.VMEM((parts, n - 1, SEQS, d), BF16),
                pltpu.VMEM((parts, SEQS, d), BF16),
                pltpu.VMEM((parts, SEQS, d), BF16),
                pltpu.VMEM((parts, n - 1, SEQS, d), BF16),
                pltpu.VMEM((n * SEQS, d), F32),
                pltpu.VMEM((parts, SEQS, d), F32),
                pltpu.VMEM((parts, n - 1, SEQS, d), BF16),
                pltpu.VMEM((parts, n - 1, SEQS, d), BF16),
                pltpu.VMEM((parts, n, SEQS, d), BF16),
                dma((SLOTS,)),
                dma((SLOTS,)),
                dma((9,)),
            ]
            + [dma((parts,))] * 8,
            compiler_params=pltpu.CompilerParams(collective_id=0, has_side_effects=True, vmem_limit_bytes=VMEM_LIMIT),
        )(
            *(
                pltpu.with_memory_space_constraint(t, pltpu.HBM)
                for t in (
                    x.reshape(n, batch // n, d), turned_round(k_cache), turned_round(v_cache), gain_a, wq, wo, gain_m,
                    w_gate, w_up, w_down, rope,
                )
            )
        )
        return out.reshape(batch, d)

    states, cache, columns, rows_of = P("dp", None), P("dp", None, "tp", None), P(None, "tp"), P("tp", None)
    return jax.shard_map(
        step,
        mesh=mesh,
        in_specs=(states, cache, cache, P(None), columns, rows_of, P(None), columns, columns, rows_of),
        out_specs=states,
        check_vma=False,
    )
```

```python
import functools

import jax
import jax.numpy as jnp
import numpy as np
from jax import lax
from jax.experimental import pallas as pl
from jax.experimental.pallas import tpu as pltpu
from jax.sharding import PartitionSpec as P

HEAD = 64
THETA = 10000
EPS = 1e-6
SEQS = 4
SLOTS = 4
TILE = 256
VMEM_LIMIT = 44 * 2**20

F32, BF16 = jnp.float32, jnp.bfloat16
MESH = pl.DeviceIdType.MESH


def dot(a, b):
    return jnp.dot(a, b, preferred_element_type=F32)


def dot_t(a, b):
    return lax.dot_general(a, b, (((1,), (1,)), ((), ())), preferred_element_type=F32)


def normed(wide, gain):
    scale = lax.rsqrt(jnp.mean(wide * wide, -1, keepdims=True) + EPS)
    return wide * scale * gain


def kernel(
    n, heads, axis,
    x_hbm, k_hbm, v_hbm, ga_hbm, wq_hbm, wo_hbm, gm_hbm, wg_hbm, wu_hbm, wd_hbm, rope_hbm,
    y_ref,
    xs, ga, gm, rope, wq, wo, wg, wu, wd,
    kbuf, vbuf, qcat, p_ref, o_ref, terms, landed, h_own, b_own, b_in, b_ref, own2, terms2, landed2, y_all,
    k_sem, v_sem, w_sem, send1, recv1, send2, recv2, send3, recv3, send4, recv4,
):
    me = lax.axis_index(axis)
    width = heads * HEAD
    rows = SEQS * heads
    batch = x_hbm.shape[0] * x_hbm.shape[1]
    steps = batch // SEQS
    parts = steps // n
    cache = k_hbm.shape[-1]
    d = x_hbm.shape[-1]

    def peer(p):
        return lax.rem(me + p, n)

    def block_of(g):
        return lax.rem(me + 1 + lax.rem(g, n), n)

    def group_of(g):
        return block_of(g) * parts + g // n

    def k_copy(g):
        return pltpu.make_async_copy(k_hbm.at[group_of(g)], kbuf.at[lax.rem(g, SLOTS)], k_sem.at[lax.rem(g, SLOTS)])

    def v_copy(g):
        return pltpu.make_async_copy(v_hbm.at[group_of(g)], vbuf.at[lax.rem(g, SLOTS)], v_sem.at[lax.rem(g, SLOTS)])

    first = [
        pltpu.make_async_copy(x_hbm, xs, w_sem.at[0]),
        pltpu.make_async_copy(ga_hbm, ga, w_sem.at[1]),
        pltpu.make_async_copy(wq_hbm, wq, w_sem.at[2]),
        pltpu.make_async_copy(rope_hbm, rope, w_sem.at[3]),
        pltpu.make_async_copy(gm_hbm, gm, w_sem.at[8]),
    ]
    wo_copy = pltpu.make_async_copy(wo_hbm, wo, w_sem.at[4])
    third = [
        pltpu.make_async_copy(wg_hbm, wg, w_sem.at[5]),
        pltpu.make_async_copy(wu_hbm, wu, w_sem.at[6]),
        pltpu.make_async_copy(wd_hbm, wd, w_sem.at[7]),
    ]

    for c in first:
        c.start()
    k_copy(0).start()
    wo_copy.start()
    v_copy(0).start()
    k_copy(1).start()

    barrier = pltpu.get_barrier_semaphore()
    for p in range(1, n):
        pl.semaphore_signal(barrier, inc=1, device_id={axis: peer(p)}, device_id_type=MESH)

    with jax.named_scope("first_wait"):
        for c in first:
            c.wait()
    v_copy(1).start()
    for g in range(2, SLOTS):
        k_copy(g).start()
        v_copy(g).start()

    a = normed(xs[...].reshape(batch, -1).astype(F32), ga[...].astype(F32)[None]).astype(BF16)
    q = dot(a, wq[...]).astype(BF16).astype(F32)
    lane = lax.broadcasted_iota(jnp.int32, q.shape, 1)
    half = HEAD // 2
    low = lax.rem(lane, HEAD) < half
    other = jnp.where(low, pltpu.roll(q, width - half, 1), pltpu.roll(q, half, 1))
    q = (q * rope[0:1, :] + other * rope[1:2, :]).astype(BF16)
    r = lax.broadcasted_iota(jnp.int32, (steps * rows, batch), 0)
    t = lax.broadcasted_iota(jnp.int32, (steps * rows, batch), 1)
    pick = jnp.where(t == (r // rows) * SEQS + lax.rem(r, SEQS), 1.0, 0.0).astype(BF16)
    r = lax.broadcasted_iota(jnp.int32, (steps * rows, width), 0)
    c = lax.broadcasted_iota(jnp.int32, (steps * rows, width), 1)
    spread = jnp.where(c // HEAD == lax.rem(r // SEQS, heads), dot(pick, q), 0.0)
    for i in range(SEQS):
        qcat[:, :, i * width : (i + 1) * width] = (
            jnp.where(lax.rem(r, SEQS) == i, spread, 0.0).astype(BF16).reshape(steps, rows, width)
        )

    row = lax.broadcasted_iota(jnp.int32, (rows, cache), 0)
    vrow = lax.broadcasted_iota(jnp.int32, (width, rows), 0)
    vcol = lax.broadcasted_iota(jnp.int32, (width, rows), 1)
    fold_r = lax.broadcasted_iota(jnp.int32, (8, rows), 0)
    fold_c = lax.broadcasted_iota(jnp.int32, (8, rows), 1)
    fold = jnp.where(lax.rem(fold_c, SEQS) == fold_r, 1.0, 0.0).astype(BF16)
    tiles = cache // TILE

    def score_pieces(g):
        slot, group = lax.rem(g, SLOTS), group_of(g)
        out = [None] * tiles

        def piece(t, i):
            x = dot(qcat[group, :, i * width : (i + 1) * width], kbuf[slot, i, :, t * TILE : (t + 1) * TILE])
            out[t] = x if out[t] is None else out[t] + x

        order = [(t, i) for u in range(0, tiles, 2) for i in range(SEQS) for t in range(u, min(u + 2, tiles))]
        return [functools.partial(piece, t, i) for t, i in order], out

    def value_pieces(g):
        slot = lax.rem(g, SLOTS)
        out = [None, None]

        def piece(c, i, t):
            x = dot_t(vbuf[slot, i, :, t * TILE : (t + 1) * TILE], p_ref[i, :, t * TILE : (t + 1) * TILE])
            out[c] = x if out[c] is None else out[c] + x

        order = [(c, c * SEQS // 2 + i, t) for i in range(SEQS // 2) for t in range(tiles) for c in range(2)]
        return [functools.partial(piece, *o) for o in order], out

    def store_weights(s):
        e = jnp.exp((s - jnp.max(s, -1, keepdims=True)) * HEAD**-0.5)
        w = e * (1.0 / jnp.sum(e, -1, keepdims=True))
        for i in range(SEQS):
            p_ref[i] = jnp.where(lax.rem(row, SEQS) == i, w, 0.0).astype(BF16)

    def folded(sums):
        acc = jnp.where(vcol // SEQS == vrow // HEAD, sums[0] + sums[1], 0.0)
        return dot_t(fold, acc.astype(BF16)).astype(BF16)

    def term1(b, k, to):
        return pltpu.make_async_remote_copy(
            terms.at[b, k], landed.at[b, k], send1.at[b], recv1.at[b, k // (n - 2)], device_id={axis: to}, device_id_type=MESH
        )

    def gather1(b, p):
        return pltpu.make_async_remote_copy(
            b_own.at[b], b_in.at[b, p - 1], send2.at[b], recv2.at[b], device_id={axis: peer(p)}, device_id_type=MESH
        )

    def term2(b, p):
        return pltpu.make_async_remote_copy(
            terms2.at[b, p - 1], landed2.at[b, p - 1], send3.at[b], recv3.at[b], device_id={axis: peer(n - p)}, device_id_type=MESH
        )

    def gather2(b, p):
        return pltpu.make_async_remote_copy(
            y_all.at[b, me], y_all.at[b, me], send4.at[b], recv4.at[b], device_id={axis: peer(p)}, device_id_type=MESH
        )

    def all_of(ref, b, send, recv):
        some = ref.at[b, pl.ds(0, n - 1)]
        return pltpu.make_async_remote_copy(some, some, send.at[b], recv.at[b], device_id={axis: me}, device_id_type=MESH)

    far_first = sorted(range(1, n), key=lambda p: -min(p, n - p))

    def finish_h(b, own):
        h = xs[me].astype(F32)[b * SEQS : (b + 1) * SEQS] + own
        with jax.named_scope(f"term1_wait#b={b}"):
            some = landed.at[b, pl.ds(0, n - 2)]
            pltpu.make_async_remote_copy(
                some, some, send1.at[b], recv1.at[b, 0], device_id={axis: me}, device_id_type=MESH
            ).wait_recv()
        for k in range(n - 2):
            h = h + landed[b, k].astype(F32)
        with jax.named_scope(f"term1_last_wait#b={b}"):
            term1(b, n - 2, me).wait_recv()
        h = h + landed[b, n - 2].astype(F32)
        h = h.astype(BF16)
        h_own[b] = h
        b_own[b] = normed(h.astype(F32), gm[...].astype(F32)[None]).astype(BF16)
        for p in far_first:
            gather1(b, p).start()

    def mlp(b):
        with jax.named_scope("gather1_wait"):
            all_of(b_in, b, send2, recv2).wait_recv()
        for j in range(n):
            b_ref[j * SEQS : (j + 1) * SEQS, :] = (b_in[b, j - 1] if j else b_own[b]).astype(F32)
        states = b_ref[...].astype(BF16)
        gate, up = dot(states, wg[...]), dot(states, wu[...])
        hidden = (gate * (1.0 / (1.0 + jnp.exp(-gate))) * up).astype(BF16)
        part = dot(hidden, wd[...])
        own2[b] = part[:SEQS]
        for j in range(1, n):
            terms2[b, j - 1] = part[j * SEQS : (j + 1) * SEQS].astype(BF16)
        for p in far_first:
            term2(b, p).start()

    def finish_y(b):
        y = h_own[b].astype(F32) + own2[b]
        with jax.named_scope("term2_wait"):
            all_of(landed2, b, send3, recv3).wait_recv()
        for p in range(1, n):
            y = y + landed2[b, p - 1].astype(F32)
        y_all[b, me] = y.astype(BF16)
        for p in far_first:
            gather2(b, p).start()

    with jax.named_scope("k0_wait"):
        k_copy(0).wait()
    todo, s = score_pieces(0)
    for piece in todo:
        piece()
    store_weights(jnp.concatenate(s, 1))
    o_ref[...] = jnp.zeros_like(o_ref)
    k_copy(SLOTS).start()
    with jax.named_scope("wo_wait"):
        wo_copy.wait()
    with jax.named_scope("barrier_wait"):
        pl.semaphore_wait(barrier, n - 1)

    def send_term(g, part):
        terms[g // n, lax.rem(g, n)] = part.astype(BF16)
        term1(g // n, lax.rem(g, n), block_of(g)).start()

    def body(g, carry):
        @pl.when(g == steps - SLOTS)
        def _():
            for c in third:
                c.start()

        with jax.named_scope("kv_wait"):
            k_copy(g + 1).wait()
            v_copy(g).wait()
        ks, s = score_pieces(g + 1)
        vs, sums = value_pieces(g)
        before = o_ref[...]
        part = []
        for j in range(len(vs)):
            for piece in ks[2 * j : 2 * j + 2]:
                piece()
            vs[j]()
            if j % 2:
                part.append(dot(before, wo[:, j // 2 * TILE : (j // 2 + 1) * TILE]))
        o_ref[...] = folded(sums)
        store_weights(jnp.concatenate(s, 1))
        part = jnp.concatenate(part, 1)[:SEQS]

        @pl.when(g + 1 + SLOTS < steps)
        def _():
            k_copy(g + 1 + SLOTS).start()

        @pl.when(g + SLOTS < steps)
        def _():
            v_copy(g + SLOTS).start()

        own_before = lax.rem(g, n) == 0

        @pl.when(jnp.logical_not(own_before))
        def _():
            send_term(g - 1, part)

        @pl.when(jnp.logical_and(own_before, g > 0))
        def _():
            finish_h(0, part)

        return carry

    lax.fori_loop(0, steps - 2, body, 0)
    g = steps - 1

    @pl.when(me >= 0)
    def _():
        with jax.named_scope("last_wait"):
            v_copy(g - 1).wait()
        vs, sums = value_pieces(g - 1)
        part = dot(o_ref[...], wo[...])[:SEQS]
        for piece in vs:
            piece()
        o_ref[...] = folded(sums)
        send_term(g - 2, part)

    @pl.when(me < n)
    def _():
        send_term(g - 1, dot(o_ref[...], wo[...])[:SEQS])
        with jax.named_scope("last_wait"):
            k_copy(g).wait()

    @pl.when(me < n + 1)
    def _():
        ks, s = score_pieces(g)
        for piece in ks:
            piece()
        store_weights(jnp.concatenate(s, 1))
        with jax.named_scope("last_v_wait"):
            v_copy(g).wait()

    @pl.when(me > -2)
    def _():
        vs, sums = value_pieces(g)
        for piece in vs:
            piece()
        o_ref[...] = folded(sums)

    @pl.when(me > -1)
    def _():
        finish_h(parts - 1, dot(o_ref[...], wo[...])[:SEQS])

    with jax.named_scope("third_wait"):
        for c in third:
            c.wait()

    def each_mlp(b, carry):
        mlp(b)
        return carry

    def each_y(b, carry):
        finish_y(b)
        return carry

    lax.fori_loop(0, parts, each_mlp, 0)
    lax.fori_loop(0, parts, each_y, 0)

    with jax.named_scope("gather2_wait"):
        for b in range(parts):
            all_of(y_all, b, send4, recv4).wait_recv()
    for j in range(n):
        y_ref[j] = jnp.concatenate([y_all[b, j].astype(F32) for b in range(parts)], 0).astype(BF16)

    with jax.named_scope("send_wait"):
        for b in range(parts):
            all_of(terms, b, send1, send1).wait_send()
            all_of(b_in, b, send2, recv2).wait_send()
            all_of(terms2, b, send3, recv3).wait_send()
            all_of(y_all, b, send4, recv4).wait_send()


def solution(mesh):
    n = mesh.shape["tp"]

    def step(x, k_cache, v_cache, gain_a, wq, wo, gain_m, w_gate, w_up, w_down):
        batch, d = x.shape
        cache, heads = k_cache.shape[1:3]
        width, ff = heads * HEAD, w_gate.shape[1]
        steps = batch // SEQS
        parts = steps // n
        rows = SEQS * heads

        def turned_round(c):
            return c.transpose(0, 2, 3, 1).reshape(steps, SEQS, width, cache)

        half = HEAD // 2
        angle = (cache - 1) * THETA ** (-np.arange(half, dtype=np.float64) / half)
        cos, sin = np.cos(angle), np.sin(angle)
        rope = np.stack([np.tile(np.concatenate([cos, cos]), heads), np.tile(np.concatenate([-sin, sin]), heads)])
        rope = jnp.asarray(rope.astype(np.float32))

        dma = pltpu.SemaphoreType.DMA
        out = pl.pallas_call(
            functools.partial(kernel, n, heads, "tp"),
            out_shape=jax.ShapeDtypeStruct((n, batch // n, d), BF16),
            in_specs=[pl.BlockSpec(memory_space=pl.ANY)] * 11,
            out_specs=pl.BlockSpec(memory_space=pltpu.VMEM),
            scratch_shapes=[
                pltpu.VMEM((n, batch // n, d), BF16),
                pltpu.VMEM((d,), BF16),
                pltpu.VMEM((d,), BF16),
                pltpu.VMEM((2, width), F32),
                pltpu.VMEM(wq.shape, BF16),
                pltpu.VMEM(wo.shape, BF16),
                pltpu.VMEM(w_gate.shape, BF16),
                pltpu.VMEM(w_up.shape, BF16),
                pltpu.VMEM(w_down.shape, BF16),
                pltpu.VMEM((SLOTS, SEQS, width, cache), BF16),
                pltpu.VMEM((SLOTS, SEQS, width, cache), BF16),
                pltpu.VMEM((steps, rows, SEQS * width), BF16),
                pltpu.VMEM((SEQS, rows, cache), BF16),
                pltpu.VMEM((8, width), BF16),
                pltpu.VMEM((parts, n - 1, SEQS, d), BF16),
                pltpu.VMEM((parts, n - 1, SEQS, d), BF16),
                pltpu.VMEM((parts, SEQS, d), BF16),
                pltpu.VMEM((parts, SEQS, d), BF16),
                pltpu.VMEM((parts, n - 1, SEQS, d), BF16),
                pltpu.VMEM((n * SEQS, d), F32),
                pltpu.VMEM((parts, SEQS, d), F32),
                pltpu.VMEM((parts, n - 1, SEQS, d), BF16),
                pltpu.VMEM((parts, n - 1, SEQS, d), BF16),
                pltpu.VMEM((parts, n, SEQS, d), BF16),
                dma((SLOTS,)),
                dma((SLOTS,)),
                dma((9,)),
            ]
            + [dma((parts,)), dma((parts, 2))]
            + [dma((parts,))] * 6,
            compiler_params=pltpu.CompilerParams(collective_id=0, has_side_effects=True, vmem_limit_bytes=VMEM_LIMIT),
        )(
            *(
                pltpu.with_memory_space_constraint(t, pltpu.HBM)
                for t in (
                    x.reshape(n, batch // n, d), turned_round(k_cache), turned_round(v_cache), gain_a, wq, wo, gain_m,
                    w_gate, w_up, w_down, rope,
                )
            )
        )
        return out.reshape(batch, d)

    states, cache, columns, rows_of = P("dp", None), P("dp", None, "tp", None), P(None, "tp"), P("tp", None)
    return jax.shard_map(
        step,
        mesh=mesh,
        in_specs=(states, cache, cache, P(None), columns, rows_of, P(None), columns, columns, rows_of),
        out_specs=states,
        check_vma=False,
    )
```
